512 devices in a mesh: dp: 64 (over x, y, core), tensor: 8 (over z).
Axes of the slice: x: 4, y: 8, z: 8, core: 2. Of those that a mesh axis runs over, the one named last changes fastest.
Arguments:
- attn_out: bfloat16 [65536, 3072], P('dp', 'tensor'), may hold values from -6 to 6
- cotangent: bfloat16 [65536, 2560], P(('dp', 'tensor')), may hold values from -0.1875 to 0.1875
- residual: bfloat16 [64, 3072, 2560], P('dp', 'tensor'), may hold values from -6 to 6
- local_offsets: int32 [64, 8, 64, 48], P('dp', 'tensor'), may hold values from 0 to 149, as said below
- local_counts: int32 [64, 8, 64], P('dp', 'tensor'), may hold values from 1 to 48, as said below
- kept_offsets: int32 [8, 64, 12], P('tensor'), may hold values from 0 to 149, as said below
- kept_counts: int32 [8, 64], P('tensor'), may hold values from 6 to 12, as said below
- bounds: int32 [65], replicated, may hold values from 0 to 7680, as said below
Outputs:
- new_residual: bfloat16 [64, 3072, 2560], P('dp', 'tensor')
- kept_sums: float32 [8, 64, 12, 128], P('tensor')
The draws below stay inside these ranges and needn't reach their ends.
Inputs may be any that keep to these rules, and one draw needn't show every extreme that they name: `local_offsets`: for each replica, band and region the 48 entries are different offsets within the region (below bounds[r + 1] - bounds[r]); slots at or past local_counts are ignored but hold such offsets too. `local_counts`: for each band, some region has 48 live slots from every replica. `kept_offsets`: for each band and region the 12 entries are different offsets within the region; slots at or past kept_counts are ignored. `kept_counts`: for each band, some region has 12 live kept slots. bounds[0] = 0, bounds[64] = 7680, rising; each region holds 90 to 150 blocks.
All inputs are finite; a program needn't handle non-finite values.
Results may differ from the reference program's by a relative error of at most 0.001.
Values may be sent and summed in bfloat16 or wider, within the bound.
A program may use at most 64 MiB of HBM per device.

```python
import jax
import jax.numpy as jnp
from jax import lax

D = 2560
HEADS = 24
HD = 128
TOK_REP = 1024
CAP = 48
GCAP = 12
TOKENS = 65536
REGION = 120
N_DP = 64
N_TENSOR = 8


def region_layout(key):
    pair_count = N_DP // 2
    widening = jax.random.randint(jax.random.fold_in(key, 101), (pair_count,), 0, REGION // 4 + 1)
    widest_pair = jax.random.randint(jax.random.fold_in(key, 107), (), 0, pair_count)
    widening = jnp.where(jnp.arange(pair_count) == widest_pair, REGION // 4, widening)
    region_sizes = jnp.stack([REGION + widening, REGION - widening], axis=1).reshape(-1).astype(jnp.int32)
    region_bounds = jnp.concatenate([jnp.zeros((1,), jnp.int32), jnp.cumsum(region_sizes).astype(jnp.int32)])
    widest = REGION + REGION // 4
    random_keys = jax.random.randint(jax.random.fold_in(key, 102), (N_TENSOR, N_DP, widest), 0, 1 << 16)
    ranked = random_keys * widest + jnp.arange(widest, dtype=jnp.int32)[None, None, :]
    shuffle = jnp.argsort(ranked, axis=-1).astype(jnp.int32)
    outside = (shuffle >= region_sizes[None, :, None]).astype(jnp.int32)
    arranged = jnp.argsort(outside * widest + jnp.arange(widest, dtype=jnp.int32)[None, None, :], axis=-1)
    shuffled = jnp.take_along_axis(shuffle, arranged, axis=-1)
    return (region_bounds, shuffled[:, :, :GCAP + CAP])


def draw_bounds(key, part):
    return region_layout(key)[0]


def draw_local_offsets(key, part):
    region_bounds, shuffled = region_layout(key)
    offset_start = jax.random.randint(jax.random.fold_in(key, 103), (N_DP, N_TENSOR, N_DP, 1), 0, GCAP)
    window_pos = offset_start + jnp.arange(CAP, dtype=jnp.int32)[None, None, None, :]
    spread_lists = jnp.broadcast_to(shuffled[None], (N_DP,) + shuffled.shape)
    return jnp.take_along_axis(spread_lists, window_pos, axis=-1).astype(jnp.int32)


def draw_local_counts(key, part):
    heat_level = jax.random.randint(jax.random.fold_in(key, 104), (N_TENSOR, N_DP), 1, 5)
    ceiling = CAP * heat_level // 4
    floor_count = jnp.maximum(ceiling // 2, 1)
    counts_drawn = jax.random.randint(jax.random.fold_in(key, 105), (N_DP, N_TENSOR, N_DP), floor_count[None], ceiling[None] + 1)
    busiest = jax.random.randint(jax.random.fold_in(key, 106), (N_TENSOR,), 0, N_DP)
    counts_drawn = jnp.where(jnp.arange(N_DP)[None, None, :] == busiest[None, :, None], CAP, counts_drawn)
    return counts_drawn.astype(jnp.int32)


def draw_kept_offsets(key, part):
    region_bounds, shuffled = region_layout(key)
    return shuffled[:, :, :GCAP].astype(jnp.int32)


def draw_kept_counts(key, part):
    counts_drawn = jax.random.randint(jax.random.fold_in(key, 108), (N_TENSOR, N_DP), GCAP // 2, GCAP + 1)
    busiest = jax.random.randint(jax.random.fold_in(key, 109), (N_TENSOR,), 0, N_DP)
    counts_drawn = jnp.where(jnp.arange(N_DP)[None, :] == busiest[:, None], GCAP, counts_drawn)
    return counts_drawn.astype(jnp.int32)


def block_levels(own_key, extent, shards, smallest, largest):
    factor_of, own = 1.0, jax.random.fold_in(own_key, 6)
    for position, parts in shards:
        steps = jnp.exp(jax.random.uniform(jax.random.fold_in(own, position), (parts,), jnp.float32, smallest / len(shards), largest / len(shards)))
        factor_of = factor_of * jnp.repeat(steps, extent[position] // parts).reshape([-1 if axis == position else 1 for axis in range(len(extent))])
    return factor_of


def scatter_about(key, shape, spread, reach, cuts=(), held_as=jnp.bfloat16):
    factor_of = block_levels(key, shape, cuts, -0.22, 0.18) if cuts else 1.0
    values = jax.random.normal(key, shape, jnp.float32) * spread * factor_of
    return jnp.minimum(jnp.maximum(values, -reach), reach).astype(held_as)


def setup_inputs(seed: int = 0) -> dict:
    key_of = jax.random.split(jax.random.key(seed), 9)
    return {
        "attn_out": scatter_about(key_of[0], (TOKENS, HEADS * HD), 1.0, 6.0, ((0, 64), (1, 8))),
        "cotangent": scatter_about(key_of[1], (TOKENS, D), TOK_REP ** -0.5, 0.1875, ((0, 512),)),
        "residual": scatter_about(key_of[2], (N_DP, HEADS * HD, D), 1.0, 6.0, ((0, 64), (1, 8))),
        "local_offsets": draw_local_offsets(jax.random.fold_in(key_of[8], 71), 0),
        "local_counts": draw_local_counts(jax.random.fold_in(key_of[8], 71), 0),
        "kept_offsets": draw_kept_offsets(jax.random.fold_in(key_of[8], 71), 0),
        "kept_counts": draw_kept_counts(jax.random.fold_in(key_of[8], 71), 0),
        "bounds": draw_bounds(jax.random.fold_in(key_of[8], 71), 0),
    }


def pick_rows(block_rows, positions):
    return block_rows[positions]


def mark_sent(positions, live_slots, block_total):
    return jnp.zeros((block_total,), jnp.float32).at[positions.reshape(-1)].max(live_slots.reshape(-1).astype(jnp.float32))


def reference(attn_out, cotangent, residual, local_offsets, local_counts, kept_offsets, kept_counts, bounds):
    attn_rows = attn_out.reshape(N_DP, TOK_REP, HEADS * HD)
    cot_rows = cotangent.reshape(N_DP, TOK_REP, D)
    region_starts = bounds[:N_DP].astype(jnp.int32)

    def replica_step(running, item):
        attn_block, cot_block, res_block, offs_block, counts_block = item
        gradient = lax.dot_general(attn_block, cot_block, (((0,), (0,)), ((), ())), preferred_element_type=jnp.float32)
        accumulated = res_block.astype(jnp.float32) + gradient
        blocks = accumulated.reshape(N_TENSOR, -1, 128)
        block_total = blocks.shape[1]
        live_slots = jnp.arange(CAP)[None, None, :] < counts_block[:, :, None]
        where_abs = (region_starts[None, :, None] + offs_block).astype(jnp.int32)
        picked = jax.vmap(pick_rows)(blocks, where_abs) * live_slots[..., None].astype(jnp.float32)
        sent_mask = jax.vmap(mark_sent, in_axes=(0, 0, None))(where_abs, live_slots, block_total)
        refreshed = (blocks * (1.0 - sent_mask[..., None])).reshape(accumulated.shape).astype(jnp.bfloat16)
        matches = (kept_offsets[:, :, :, None] == offs_block[:, :, None, :]).astype(jnp.float32)
        running = running + jnp.einsum("trji,tric->trjc", matches, picked, precision=lax.Precision.HIGHEST)
        return running, refreshed

    empty_sums = jnp.zeros((N_TENSOR, N_DP, GCAP, 128), jnp.float32)
    summed_all, new_residual = lax.scan(replica_step, empty_sums, (attn_rows, cot_rows, residual, local_offsets, local_counts))
    kept_live = (jnp.arange(GCAP)[None, None, :] < kept_counts[:, :, None]).astype(jnp.float32)
    kept_sums = summed_all * kept_live[..., None]
    return new_residual, kept_sums
```

```python
import functools

import jax
import jax.numpy as jnp
from jax import lax
from jax.experimental import pallas as pl
from jax.experimental.pallas import tpu as pltpu
from jax.sharding import PartitionSpec as P

MESH = pl.DeviceIdType.MESH
BLK = 128
CHUNK = 512
KEPT = 12
F32 = jnp.float32
BF16 = jnp.bfloat16


def kernel(
    cfg,
    attn_hbm, cot_hbm, res_hbm, lo_ref, lc_ref, ko_ref, kc_ref, bounds_ref,
    new_hbm, kept_ref,
    attn_v, own_v, res_v, new_v, at_own, at_pair, at_far, pair, far, acc,
    rho, kappa, hit, idx_v, idx_s,
    contrib, partner_in, share, gathered, totals,
    load_sem, idx_sem, store_sem, ring_send, ring_recv,
    pair_send, pair_recv, rs_send, rs_extra, rs_recv, ag_send, ag_recv, swap_send, swap_recv,
):
    chips, n_z = cfg["chips"], cfg["n_z"]
    half = chips // 2
    n_pair = n_z // 2 - 1
    rows = attn_hbm.shape[1]
    width = cot_hbm.shape[1]
    tokens = cot_hbm.shape[0]
    quarters = width // CHUNK
    per_chunk = CHUNK // BLK
    n_cols = width // BLK
    regions = 2 * chips
    magic = -(-(1 << 20) // n_cols)
    tiles = regions * KEPT // 8
    own_tiles = tiles // chips
    half_tiles = tiles // 2

    dp = lax.axis_index("dp")
    z = lax.axis_index("tensor")
    chip = dp // 2
    core = lax.rem(dp, 2)
    right = lax.rem(z + 1, n_z)
    left = lax.rem(z + n_z - 1, n_z)
    partner = dp + 1 - 2 * core
    lane_row = lax.rem(chip, half)
    owner = chip // half == core

    loads = [
        pltpu.make_async_copy(attn_hbm, attn_v, load_sem.at[0]),
    ]
    for q in range(quarters):
        cols = pl.ds(q * CHUNK, CHUNK)
        loads.append(pltpu.make_async_copy(cot_hbm.at[:, cols], own_v.at[q], load_sem.at[1 + q]))
        loads.append(
            pltpu.make_async_copy(res_hbm.at[:, cols], res_v.at[q], load_sem.at[1 + quarters + q])
        )
    for copy in loads:
        copy.start()

    barrier = pltpu.get_barrier_semaphore()
    for to in (left, right):
        pl.semaphore_signal(
            barrier, inc=1, device_id={"dp": dp, "tensor": to}, device_id_type=MESH
        )
    pl.semaphore_signal(
        barrier, inc=1, device_id={"dp": partner, "tensor": z}, device_id_type=MESH
    )

    def greet(j, carry):
        peer = lax.rem(chip + j, chips)
        pl.semaphore_signal(
            barrier, inc=1, device_id={"dp": 2 * peer + core, "tensor": z}, device_id_type=MESH
        )
        return carry

    lax.fori_loop(1, chips, greet, 0)
    pl.semaphore_wait(barrier, chips + 2)

    def hop(side, step, q):
        to = right if side == 0 else left
        if step == 1:
            src = cot_hbm.at[:, pl.ds(pl.multiple_of(q * CHUNK, CHUNK), CHUNK)]
        elif step <= n_pair:
            src = pair.at[step - 2, q, pl.ds(side * tokens, tokens)]
        else:
            src = pair.at[
                step - 2, q, pl.ds(side * tokens + side * (tokens // 2), tokens // 2)
            ]
        if step <= n_pair:
            dst = pair.at[step - 1, q, pl.ds(side * tokens, tokens)]
        else:
            dst = far.at[q, pl.ds(side * (tokens // 2), tokens // 2)]
        return pltpu.make_async_remote_copy(
            src_ref=src,
            dst_ref=dst,
            send_sem=ring_send.at[side, step - 1, q],
            recv_sem=ring_recv.at[side, step - 1, q],
            device_id={"dp": dp, "tensor": to},
            device_id_type=MESH,
        )

    def first(q, carry):
        hop(0, 1, q).start()
        hop(1, 1, q).start()
        return carry

    lax.fori_loop(0, quarters, first, 0)

    offsets = lo_ref[...]
    live = lax.broadcasted_iota(jnp.int32, offsets.shape, 0) < lc_ref[...]
    starts = bounds_ref[:, 0:regions]
    where_abs = starts + offsets
    where_row = (where_abs * magic) >> 20
    where_col = where_abs - where_row * n_cols
    rho[...] = jnp.full(rho.shape, -1, jnp.int32)
    kappa[...] = jnp.full(kappa.shape, -1, jnp.int32)
    rho[0:regions, 0 : offsets.shape[0]] = jnp.where(live, where_row, -1).T
    kappa[0:regions, 0 : offsets.shape[0]] = where_col.T
    hit[...] = jnp.zeros(hit.shape, F32)

    sent = jnp.where(live, offsets, -1)
    idx_v[...] = jnp.zeros(idx_v.shape, jnp.int32)
    nowhere = rows * n_cols
    for j in range(KEPT):
        wanted = ko_ref[j]
        same = jnp.where(sent == wanted, 1, 0)
        found = jnp.sum(same, axis=0, keepdims=True) * jnp.where(j < kc_ref[...], 1, 0)
        kept_abs = starts + wanted
        kept_row = (kept_abs * magic) >> 20
        position = (kept_abs - kept_row * n_cols) * rows + kept_row
        idx_v[j : j + 1, 0:regions] = jnp.where(found > 0, position, nowhere)
    acc[nowhere : nowhere + 8, :] = jnp.zeros((8, BLK), F32)

    loads[0].wait()

    def turned(source):
        start = pl.multiple_of(source * tokens, tokens)
        return attn_v[pl.ds(start, tokens), :].astype(F32).T.astype(BF16)

    at_own[...] = turned(z)
    index_copy = pltpu.make_async_copy(idx_v, idx_s, idx_sem)
    index_copy.start()

    def accumulate(q, lhs, rhs_ref, start):
        for part in range(CHUNK // 256):
            got = jnp.dot(
                lhs, rhs_ref[:, part * 256 : part * 256 + 256], preferred_element_type=F32
            )
            for b in range(2):
                place = pl.ds(
                    pl.multiple_of((q * per_chunk + part * 2 + b) * rows, rows), rows
                )
                block = got[:, b * BLK : b * BLK + BLK]
                if start is None:
                    acc[place, :] = acc[place, :] + block
                else:
                    col = (part * 2 + b) * BLK
                    acc[place, :] = start[:, col : col + BLK].astype(F32) + block

    for copy in loads[1:]:
        copy.wait()

    def own_step(q, carry):
        accumulate(q, at_own[...], own_v.at[q], res_v.at[q])
        return carry

    lax.fori_loop(0, quarters, own_step, 0)
    for d in range(1, n_pair + 1):
        at_pair[d - 1, :, 0:tokens] = turned(lax.rem(z + n_z - d, n_z))
        at_pair[d - 1, :, tokens : 2 * tokens] = turned(lax.rem(z + d, n_z))
    at_far[...] = turned(lax.rem(z + n_z // 2, n_z))

    mask_loops = range(2, n_pair + 1) if n_pair > 1 else range(1, n_pair + 1)
    per_visit = -(-regions // (quarters * len(mask_loops)))
    row_of = lax.broadcasted_iota(jnp.int32, (rows, BLK), 0)
    col_of = lax.broadcasted_iota(jnp.int32, (BLK, BLK), 0)

    def mark(visit):
        total = hit[...]
        for i in range(per_visit):
            r = visit * per_visit + i
            in_row = jnp.where(row_of == rho[pl.ds(r, 1), :], 1.0, 0.0).astype(BF16)
            in_col = jnp.where(col_of == kappa[pl.ds(r, 1), :], 1.0, 0.0).astype(BF16)
            total = total + lax.dot_general(
                in_row, in_col, (((1,), (1,)), ((), ())), preferred_element_type=F32
            )
        hit[...] = total

    for d in range(1, n_pair + 1):

        def pair_step(q, carry, d=d):
            hop(0, d, q).wait_recv()
            hop(0, d + 1, q).start()
            hop(1, d, q).wait_recv()
            hop(1, d + 1, q).start()
            accumulate(q, at_pair[d - 1], pair.at[d - 1, q], None)
            if d in mask_loops:
                mark((d - mask_loops[0]) * quarters + q)
            return carry

        lax.fori_loop(0, quarters, pair_step, 0)

    def far_step(q, carry):
        hop(0, n_pair + 1, q).wait_recv()
        hop(1, n_pair + 1, q).wait_recv()
        accumulate(q, at_far[...], far.at[q], None)
        return carry

    index_copy.wait()
    lax.fori_loop(0, quarters, far_step, 0)

    def pick(tile, carry):
        first = tile * 8
        j = first // regions
        for m in range(8):
            at = idx_s[j, first - j * regions + m]
            at = jnp.minimum(jnp.maximum(at, 0), nowhere)
            contrib[tile, m : m + 1, :] = acc[pl.ds(at, 1), :]
        return carry

    lax.fori_loop(0, tiles, pick, 0)

    mine = core * half_tiles
    theirs = (1 - core) * half_tiles
    to_partner = pltpu.make_async_remote_copy(
        src_ref=contrib.at[pl.ds(theirs, half_tiles)],
        dst_ref=partner_in,
        send_sem=pair_send,
        recv_sem=pair_recv,
        device_id={"dp": partner, "tensor": z},
        device_id_type=MESH,
    )
    to_partner.start()
    to_partner.wait_recv()

    def add_partner(k, carry):
        share[k] = contrib[mine + k] + partner_in[k]
        return carry

    lax.fori_loop(0, half_tiles, add_partner, 0)

    def scatter(j, send_sem):
        slot = lax.rem(lane_row + j, half)
        return pltpu.make_async_remote_copy(
            src_ref=share.at[pl.ds(slot * own_tiles, own_tiles)],
            dst_ref=gathered.at[chip],
            send_sem=send_sem,
            recv_sem=rs_recv,
            device_id={"dp": 2 * (core * half + slot) + core, "tensor": z},
            device_id_type=MESH,
        )

    def scatter_step(j, carry):
        scatter(j, rs_send).start()
        return carry

    @pl.when(jnp.logical_not(owner))
    def _():
        scatter(0, rs_extra).start()

    lax.fori_loop(1, half, scatter_step, 0)

    for c in range(n_cols):
        keep = hit[:, c : c + 1] < 0.5
        value = acc[c * rows : (c + 1) * rows, :]
        new_v[:, c * BLK : (c + 1) * BLK] = jnp.where(keep, value, 0.0).astype(BF16)
    write = pltpu.make_async_copy(new_v, new_hbm, store_sem)
    write.start()

    def hand_out(j):
        return pltpu.make_async_remote_copy(
            src_ref=totals.at[pl.ds(chip * own_tiles, own_tiles)],
            dst_ref=totals.at[pl.ds(chip * own_tiles, own_tiles)],
            send_sem=ag_send,
            recv_sem=ag_recv,
            device_id={"dp": 2 * lax.rem(chip + j, chips) + core, "tensor": z},
            device_id_type=MESH,
        )

    def hand_step(j, carry):
        hand_out(j).start()
        return carry

    def wait_for(ref, count, sem):
        if count == 0:
            return
        part = ref.at[pl.ds(0, count)]
        pltpu.make_async_copy(part, part, sem).wait()

    @pl.when(owner)
    def _():
        gathered[chip] = share[pl.ds(lane_row * own_tiles, own_tiles)]
        wait_for(gathered, chips - 1, rs_recv)
        total = gathered[0]
        for k in range(1, chips):
            total = total + gathered[k]
        totals[pl.ds(chip * own_tiles, own_tiles)] = total
        lax.fori_loop(1, chips, hand_step, 0)
        wait_for(totals, (half - 1) * own_tiles, ag_recv)

    @pl.when(jnp.logical_not(owner))
    def _():
        wait_for(totals, half_tiles, ag_recv)

    swap = pltpu.make_async_remote_copy(
        src_ref=totals.at[pl.ds(mine, half_tiles)],
        dst_ref=totals.at[pl.ds(mine, half_tiles)],
        send_sem=swap_send,
        recv_sem=swap_recv,
        device_id={"dp": partner, "tensor": z},
        device_id_type=MESH,
    )
    swap.start()

    for d in range(1, n_pair + 2):

        def sent_step(q, carry, d=d):
            hop(0, d, q).wait_send()
            hop(1, d, q).wait_send()
            return carry

        lax.fori_loop(0, quarters, sent_step, 0)
    to_partner.wait_send()
    wait_for(share, (half - 1) * own_tiles, rs_send)

    @pl.when(jnp.logical_not(owner))
    def _():
        scatter(0, rs_extra).wait_send()

    @pl.when(owner)
    def _():
        wait_for(totals, (chips - 1) * own_tiles, ag_send)

    write.wait()
    swap.wait()
    kept_ref[...] = totals[...]


def on_device(
    attn_out, cotangent, residual, local_offsets, local_counts, kept_offsets, kept_counts, bounds
):
    n_dp, n_z = lax.axis_size("dp"), lax.axis_size("tensor")
    chips = n_dp // 2
    tokens, width = cotangent.shape
    rows = attn_out.shape[1]
    regions = local_offsets.shape[2]
    n_pair = n_z // 2 - 1
    quarters = width // CHUNK
    n_cols = width // BLK
    padded = -(-regions // 8) * 8 + 8 * quarters
    anywhere = pl.BlockSpec(memory_space=pl.ANY)
    vmem = pl.BlockSpec(memory_space=pltpu.VMEM)
    dma = pltpu.SemaphoreType.DMA
    tiles = regions * KEPT // 8
    new, kept = pl.pallas_call(
        functools.partial(kernel, {"chips": chips, "n_z": n_z}),
        out_shape=(
            jax.ShapeDtypeStruct((rows, width), BF16),
            jax.ShapeDtypeStruct((tiles, 8, BLK), F32),
        ),
        in_specs=[anywhere] * 3 + [vmem] * 5,
        out_specs=(anywhere, vmem),
        scratch_shapes=[
            pltpu.VMEM(attn_out.shape, BF16),
            pltpu.VMEM((quarters, tokens, CHUNK), BF16),
            pltpu.VMEM((quarters, rows, CHUNK), BF16),
            pltpu.VMEM((rows, width), BF16),
            pltpu.VMEM((rows, tokens), BF16),
            pltpu.VMEM((n_pair, rows, 2 * tokens), BF16),
            pltpu.VMEM((rows, tokens), BF16),
            pltpu.VMEM((n_pair, quarters, 2 * tokens, CHUNK), BF16),
            pltpu.VMEM((quarters, tokens, CHUNK), BF16),
            pltpu.VMEM((rows * n_cols + 8, BLK), F32),
            pltpu.VMEM((padded, BLK), jnp.int32),
            pltpu.VMEM((padded, BLK), jnp.int32),
            pltpu.VMEM((rows, BLK), F32),
            pltpu.VMEM((16, BLK), jnp.int32),
            pltpu.SMEM((16, BLK), jnp.int32),
            pltpu.VMEM((tiles, 8, BLK), F32),
            pltpu.VMEM((tiles // 2, 8, BLK), F32),
            pltpu.VMEM((tiles // 2, 8, BLK), F32),
            pltpu.VMEM((chips, tiles // chips, 8, BLK), F32),
            pltpu.VMEM((tiles, 8, BLK), F32),
            dma((1 + 2 * quarters,)),
            dma,
            dma,
            dma((2, n_pair + 1, quarters)),
            dma((2, n_pair + 1, quarters)),
            dma,
            dma,
            dma,
            dma,
            dma,
            dma,
            dma,
            dma,
            dma,
        ],
        compiler_params=pltpu.CompilerParams(collective_id=0, has_side_effects=True),
    )(
        attn_out,
        cotangent,
        residual[0],
        local_offsets[0, 0].T,
        local_counts[0],
        kept_offsets.transpose(2, 0, 1),
        kept_counts,
        bounds[None],
    )
    return new[None], kept.reshape(KEPT, regions, BLK).transpose(1, 0, 2)[None]


def solution(mesh):
    in_specs = (
        P("dp", "tensor"),
        P(("dp", "tensor"), None),
        P("dp", "tensor", None),
        P("dp", "tensor", None, None),
        P("dp", "tensor", None),
        P("tensor", None, None),
        P("tensor", None),
        P(),
    )
    out_specs = (P("dp", "tensor", None), P("tensor", None, None, None))
    return jax.shard_map(
        on_device, mesh=mesh, in_specs=in_specs, out_specs=out_specs, check_vma=False
    )
```

```python
import functools

import jax
import jax.numpy as jnp
from jax import lax
from jax.experimental import pallas as pl
from jax.experimental.pallas import tpu as pltpu
from jax.sharding import PartitionSpec as P

MESH = pl.DeviceIdType.MESH
BLK = 128
CHUNK = 512
KEPT = 12
GRID_Y = 8
F32 = jnp.float32
BF16 = jnp.bfloat16


def kernel(
    cfg,
    attn_hbm, cot_hbm, res_hbm, lo_ref, lc_ref, ko_ref, kc_ref, bounds_ref,
    new_hbm, kept_hbm,
    attn_v, own_v, res_v, new_v, at_own, at_pair, at_far, pair, far, acc,
    rho, kappa, hit, idx_v, idx_s,
    contrib, partner_in, share, gathered, totals,
    load_sem, idx_sem, store_sem, ring_send, ring_recv,
    word, pair_send, pair_recv, rs_send, rs_extra, rs_recv, ag_send, ag_recv, swap_send, swap_recv,
):
    chips, n_z = cfg["chips"], cfg["n_z"]
    half = chips // 2
    n_pair = n_z // 2 - 1
    rows = attn_hbm.shape[1]
    width = cot_hbm.shape[1]
    tokens = cot_hbm.shape[0]
    quarters = width // CHUNK
    per_chunk = CHUNK // BLK
    n_cols = width // BLK
    regions = 2 * chips
    magic = -(-(1 << 20) // n_cols)
    tiles = regions * KEPT // 8
    own_tiles = tiles // chips
    half_tiles = tiles // 2

    dp = lax.axis_index("dp")
    z = lax.axis_index("tensor")
    chip = dp // 2
    core = lax.rem(dp, 2)
    right = lax.rem(z + 1, n_z)
    left = lax.rem(z + n_z - 1, n_z)
    partner = dp + 1 - 2 * core
    lane_row = lax.rem(chip, half)
    owner = chip // half == core
    n_x, n_y = cfg["n_x"], cfg["n_y"]
    x, y = chip // n_y, lax.rem(chip, n_y)
    near_x = [lax.rem(x + step, n_x) * n_y + y for step in sorted({1, n_x - 1}) if n_x > 1]
    near_y = [x * n_y + lax.rem(y + step, n_y) for step in sorted({1, n_y - 1}) if n_y > 1]

    stages = [near_x] * max(n_x // 2 - 1, 0) + [near_y] * (n_y // 2)

    def pass_word(stage):
        if 0 < stage <= len(stages):
            pl.semaphore_wait(word.at[stage - 1], len(stages[stage - 1]))
        if stage < len(stages):
            tell(word.at[stage], stages[stage])


    loads = [
        pltpu.make_async_copy(attn_hbm, attn_v, load_sem.at[0]),
    ]
    for q in range(quarters):
        cols = pl.ds(q * CHUNK, CHUNK)
        loads.append(pltpu.make_async_copy(cot_hbm.at[:, cols], own_v.at[q], load_sem.at[1 + q]))
        loads.append(
            pltpu.make_async_copy(res_hbm.at[:, cols], res_v.at[q], load_sem.at[1 + quarters + q])
        )
    for copy in loads:
        copy.start()

    barrier = pltpu.get_barrier_semaphore()
    for to in (left, right):
        pl.semaphore_signal(
            barrier, inc=1, device_id={"dp": dp, "tensor": to}, device_id_type=MESH
        )
    pl.semaphore_signal(
        barrier, inc=1, device_id={"dp": partner, "tensor": z}, device_id_type=MESH
    )

    def tell(sem, near):
        for to in near:
            pl.semaphore_signal(
                sem, inc=1, device_id={"dp": 2 * to + core, "tensor": z}, device_id_type=MESH
            )

    tell(barrier, near_x + near_y)
    pl.semaphore_wait(barrier, 3 + len(near_x) + len(near_y))

    def hop(side, step, q):
        to = right if side == 0 else left
        if step == 1:
            src = cot_hbm.at[:, pl.ds(pl.multiple_of(q * CHUNK, CHUNK), CHUNK)]
        elif step <= n_pair:
            src = pair.at[step - 2, q, pl.ds(side * tokens, tokens)]
        else:
            src = pair.at[
                step - 2, q, pl.ds(side * tokens + side * (tokens // 2), tokens // 2)
            ]
        if step <= n_pair:
            dst = pair.at[step - 1, q, pl.ds(side * tokens, tokens)]
        else:
            dst = far.at[q, pl.ds(side * (tokens // 2), tokens // 2)]
        return pltpu.make_async_remote_copy(
            src_ref=src,
            dst_ref=dst,
            send_sem=ring_send.at[side, step - 1, q],
            recv_sem=ring_recv.at[side, step - 1, q],
            device_id={"dp": dp, "tensor": to},
            device_id_type=MESH,
        )

    def first(q, carry):
        hop(0, 1, q).start()
        hop(1, 1, q).start()
        return carry

    lax.fori_loop(0, quarters, first, 0)

    pass_word(0)

    offsets = lo_ref[...]
    live = lax.broadcasted_iota(jnp.int32, offsets.shape, 0) < lc_ref[...]
    starts = bounds_ref[:, 0:regions]
    where_abs = starts + offsets
    where_row = (where_abs * magic) >> 20
    where_col = where_abs - where_row * n_cols
    rho[...] = jnp.full(rho.shape, -1, jnp.int32)
    kappa[...] = jnp.full(kappa.shape, -1, jnp.int32)
    rho[0:regions, 0 : offsets.shape[0]] = jnp.where(live, where_row, -1).T
    kappa[0:regions, 0 : offsets.shape[0]] = where_col.T
    hit[...] = jnp.zeros(hit.shape, F32)

    sent = jnp.where(live, offsets, -1)
    idx_v[...] = jnp.zeros(idx_v.shape, jnp.int32)
    nowhere = rows * n_cols
    for j in range(KEPT):
        wanted = ko_ref[j]
        same = jnp.where(sent == wanted, 1, 0)
        found = jnp.sum(same, axis=0, keepdims=True) * jnp.where(j < kc_ref[...], 1, 0)
        kept_abs = starts + wanted
        kept_row = (kept_abs * magic) >> 20
        position = (kept_abs - kept_row * n_cols) * rows + kept_row
        idx_v[j : j + 1, 0:regions] = jnp.where(found > 0, position, nowhere)
    acc[nowhere : nowhere + 8, :] = jnp.zeros((8, BLK), F32)

    pass_word(1)

    loads[0].wait()

    def turned(source):
        start = pl.multiple_of(source * tokens, tokens)
        return attn_v[pl.ds(start, tokens), :].astype(F32).T.astype(BF16)

    at_own[...] = turned(z)
    index_copy = pltpu.make_async_copy(idx_v, idx_s, idx_sem)
    index_copy.start()

    def accumulate(q, lhs, rhs_ref, start):
        for part in range(CHUNK // 256):
            got = jnp.dot(
                lhs, rhs_ref[:, part * 256 : part * 256 + 256], preferred_element_type=F32
            )
            for b in range(2):
                place = pl.ds(
                    pl.multiple_of((q * per_chunk + part * 2 + b) * rows, rows), rows
                )
                block = got[:, b * BLK : b * BLK + BLK]
                if start is None:
                    acc[place, :] = acc[place, :] + block
                else:
                    col = (part * 2 + b) * BLK
                    acc[place, :] = start[:, col : col + BLK].astype(F32) + block

    for copy in loads[1:]:
        copy.wait()

    def own_step(q, carry):
        accumulate(q, at_own[...], own_v.at[q], res_v.at[q])
        return carry

    lax.fori_loop(0, quarters, own_step, 0)
    pass_word(2)
    for d in range(1, n_pair + 1):
        at_pair[d - 1, :, 0:tokens] = turned(lax.rem(z + n_z - d, n_z))
        at_pair[d - 1, :, tokens : 2 * tokens] = turned(lax.rem(z + d, n_z))
    at_far[...] = turned(lax.rem(z + n_z // 2, n_z))

    mask_loops = range(2, n_pair + 1) if n_pair > 1 else range(1, n_pair + 1)
    per_visit = -(-regions // (quarters * len(mask_loops)))
    row_of = lax.broadcasted_iota(jnp.int32, (rows, BLK), 0)
    col_of = lax.broadcasted_iota(jnp.int32, (BLK, BLK), 0)

    def mark(visit):
        total = hit[...]
        for i in range(per_visit):
            r = visit * per_visit + i
            in_row = jnp.where(row_of == rho[pl.ds(r, 1), :], 1.0, 0.0).astype(BF16)
            in_col = jnp.where(col_of == kappa[pl.ds(r, 1), :], 1.0, 0.0).astype(BF16)
            total = total + lax.dot_general(
                in_row, in_col, (((1,), (1,)), ((), ())), preferred_element_type=F32
            )
        hit[...] = total

    for d in range(1, n_pair + 1):

        def pair_step(q, carry, d=d):
            hop(0, d, q).wait_recv()
            hop(0, d + 1, q).start()
            hop(1, d, q).wait_recv()
            hop(1, d + 1, q).start()
            accumulate(q, at_pair[d - 1], pair.at[d - 1, q], None)
            if d in mask_loops:
                mark((d - mask_loops[0]) * quarters + q)
            return carry

        pass_word(d + 2)
        lax.fori_loop(0, quarters, pair_step, 0)

    def far_step(q, carry):
        hop(0, n_pair + 1, q).wait_recv()
        hop(1, n_pair + 1, q).wait_recv()
        accumulate(q, at_far[...], far.at[q], None)
        return carry

    for stage in range(n_pair + 3, len(stages) + 1):
        pass_word(stage)
    index_copy.wait()
    lax.fori_loop(0, quarters, far_step, 0)

    def pick(tile, carry):
        first = tile * 8
        j = first // regions
        for m in range(8):
            at = idx_s[j, first - j * regions + m]
            at = jnp.minimum(jnp.maximum(at, 0), nowhere)
            contrib[tile, m : m + 1, :] = acc[pl.ds(at, 1), :]
        return carry

    lax.fori_loop(0, tiles, pick, 0)

    mine = core * half_tiles
    theirs = (1 - core) * half_tiles
    to_partner = pltpu.make_async_remote_copy(
        src_ref=contrib.at[pl.ds(theirs, half_tiles)],
        dst_ref=partner_in,
        send_sem=pair_send,
        recv_sem=pair_recv,
        device_id={"dp": partner, "tensor": z},
        device_id_type=MESH,
    )
    to_partner.start()
    to_partner.wait_recv()

    def add_partner(k, carry):
        share[k] = contrib[mine + k] + partner_in[k]
        return carry

    lax.fori_loop(0, half_tiles, add_partner, 0)

    def scatter(j, send_sem):
        slot = lax.rem(lane_row + j, half)
        return pltpu.make_async_remote_copy(
            src_ref=share.at[pl.ds(slot * own_tiles, own_tiles)],
            dst_ref=gathered.at[chip],
            send_sem=send_sem,
            recv_sem=rs_recv,
            device_id={"dp": 2 * (core * half + slot) + core, "tensor": z},
            device_id_type=MESH,
        )

    def scatter_step(j, carry):
        scatter(j, rs_send).start()
        return carry

    @pl.when(jnp.logical_not(owner))
    def _():
        scatter(0, rs_extra).start()

    lax.fori_loop(1, half, scatter_step, 0)

    for c in range(n_cols):
        keep = hit[:, c : c + 1] < 0.5
        value = acc[c * rows : (c + 1) * rows, :]
        new_v[:, c * BLK : (c + 1) * BLK] = jnp.where(keep, value, 0.0).astype(BF16)
    write = pltpu.make_async_copy(new_v, new_hbm, store_sem)
    write.start()

    def hand_out(j):
        return pltpu.make_async_remote_copy(
            src_ref=totals.at[pl.ds(chip * own_tiles, own_tiles)],
            dst_ref=totals.at[pl.ds(chip * own_tiles, own_tiles)],
            send_sem=ag_send,
            recv_sem=ag_recv,
            device_id={"dp": 2 * lax.rem(chip + j, chips) + core, "tensor": z},
            device_id_type=MESH,
        )

    def hand_step(j, carry):
        hand_out(j).start()
        return carry

    def wait_for(ref, count, sem):
        if count == 0:
            return
        part = ref.at[pl.ds(0, count)]
        pltpu.make_async_copy(part, part, sem).wait()

    @pl.when(owner)
    def _():
        gathered[chip] = share[pl.ds(lane_row * own_tiles, own_tiles)]
        wait_for(gathered, chips - 1, rs_recv)
        total = gathered[0]
        for k in range(1, chips):
            total = total + gathered[k]
        totals[pl.ds(chip * own_tiles, own_tiles)] = total
        lax.fori_loop(1, chips, hand_step, 0)
        wait_for(totals, (half - 1) * own_tiles, ag_recv)

    @pl.when(jnp.logical_not(owner))
    def _():
        wait_for(totals, half_tiles, ag_recv)

    swap = pltpu.make_async_remote_copy(
        src_ref=totals.at[pl.ds(mine, half_tiles)],
        dst_ref=totals.at[pl.ds(mine, half_tiles)],
        send_sem=swap_send,
        recv_sem=swap_recv,
        device_id={"dp": partner, "tensor": z},
        device_id_type=MESH,
    )
    swap.start()

    for d in range(1, n_pair + 2):

        def sent_step(q, carry, d=d):
            hop(0, d, q).wait_send()
            hop(1, d, q).wait_send()
            return carry

        lax.fori_loop(0, quarters, sent_step, 0)
    to_partner.wait_send()
    wait_for(share, (half - 1) * own_tiles, rs_send)

    @pl.when(jnp.logical_not(owner))
    def _():
        scatter(0, rs_extra).wait_send()

    @pl.when(owner)
    def _():
        wait_for(totals, (chips - 1) * own_tiles, ag_send)

    write.wait()
    swap.wait()
    keep_out = pltpu.make_async_copy(totals, kept_hbm, store_sem)
    keep_out.start()
    keep_out.wait()


def finish(new_ref, kept_ref, new_out, kept_out, new_v, kept_v, sem_in, sem_out):
    pieces = new_v.shape[0]
    each = new_ref.shape[0] // pieces
    moves = [(kept_ref, kept_v, kept_out)]
    for i in range(pieces):
        part = pl.ds(i * each, each)
        moves.append((new_ref.at[part], new_v.at[i], new_out.at[part]))
    inward = [
        pltpu.make_async_copy(a, b, sem_in.at[i]) for i, (a, b, _) in enumerate(moves)
    ]
    outward = [
        pltpu.make_async_copy(b, c, sem_out.at[i]) for i, (_, b, c) in enumerate(moves)
    ]
    for copy in inward:
        copy.start()
    for got, put in zip(inward, outward):
        got.wait()
        put.start()
    for put in outward:
        put.wait()


def on_device(
    attn_out, cotangent, residual, local_offsets, local_counts, kept_offsets, kept_counts, bounds
):
    n_dp, n_z = lax.axis_size("dp"), lax.axis_size("tensor")
    chips = n_dp // 2
    n_y = GRID_Y if chips % GRID_Y == 0 else chips
    n_x = chips // n_y
    tokens, width = cotangent.shape
    rows = attn_out.shape[1]
    regions = local_offsets.shape[2]
    n_pair = n_z // 2 - 1
    quarters = width // CHUNK
    n_cols = width // BLK
    padded = -(-regions // 8) * 8 + 8 * quarters
    anywhere = pl.BlockSpec(memory_space=pl.ANY)
    vmem = pl.BlockSpec(memory_space=pltpu.VMEM)
    dma = pltpu.SemaphoreType.DMA
    tiles = regions * KEPT // 8
    new, kept = pl.pallas_call(
        functools.partial(kernel, {"chips": chips, "n_z": n_z, "n_x": n_x, "n_y": n_y}),
        out_shape=(
            jax.ShapeDtypeStruct((rows, width), BF16),
            jax.ShapeDtypeStruct((tiles, 8, BLK), F32),
        ),
        in_specs=[anywhere] * 3 + [vmem] * 5,
        out_specs=(anywhere, anywhere),
        scratch_shapes=[
            pltpu.VMEM(attn_out.shape, BF16),
            pltpu.VMEM((quarters, tokens, CHUNK), BF16),
            pltpu.VMEM((quarters, rows, CHUNK), BF16),
            pltpu.VMEM((rows, width), BF16),
            pltpu.VMEM((rows, tokens), BF16),
            pltpu.VMEM((n_pair, rows, 2 * tokens), BF16),
            pltpu.VMEM((rows, tokens), BF16),
            pltpu.VMEM((n_pair, quarters, 2 * tokens, CHUNK), BF16),
            pltpu.VMEM((quarters, tokens, CHUNK), BF16),
            pltpu.VMEM((rows * n_cols + 8, BLK), F32),
            pltpu.VMEM((padded, BLK), jnp.int32),
            pltpu.VMEM((padded, BLK), jnp.int32),
            pltpu.VMEM((rows, BLK), F32),
            pltpu.VMEM((16, BLK), jnp.int32),
            pltpu.SMEM((16, BLK), jnp.int32),
            pltpu.VMEM((tiles, 8, BLK), F32),
            pltpu.VMEM((tiles // 2, 8, BLK), F32),
            pltpu.VMEM((tiles // 2, 8, BLK), F32),
            pltpu.VMEM((chips, tiles // chips, 8, BLK), F32),
            pltpu.VMEM((tiles, 8, BLK), F32),
            dma((1 + 2 * quarters,)),
            dma,
            dma,
            dma((2, n_pair + 1, quarters)),
            dma((2, n_pair + 1, quarters)),
            pltpu.SemaphoreType.REGULAR((n_x + n_y,)),
            dma,
            dma,
            dma,
            dma,
            dma,
            dma,
            dma,
            dma,
            dma,
        ],
        compiler_params=pltpu.CompilerParams(collective_id=0, has_side_effects=True),
    )(
        attn_out,
        cotangent,
        residual[0],
        local_offsets[0, 0].T,
        local_counts[0],
        kept_offsets.transpose(2, 0, 1),
        kept_counts,
        bounds[None],
    )
    pieces = 4
    new, kept = pl.pallas_call(
        finish,
        out_shape=(
            jax.ShapeDtypeStruct(new.shape, BF16),
            jax.ShapeDtypeStruct(kept.shape, F32),
        ),
        in_specs=[anywhere] * 2,
        out_specs=(anywhere, anywhere),
        scratch_shapes=[
            pltpu.VMEM((pieces, rows // pieces, width), BF16),
            pltpu.VMEM(kept.shape, F32),
            dma((pieces + 1,)),
            dma((pieces + 1,)),
        ],
    )(new, kept)
    return new[None], kept.reshape(KEPT, regions, BLK).transpose(1, 0, 2)[None]


def solution(mesh):
    in_specs = (
        P("dp", "tensor"),
        P(("dp", "tensor"), None),
        P("dp", "tensor", None),
        P("dp", "tensor", None, None),
        P("dp", "tensor", None),
        P("tensor", None, None),
        P("tensor", None),
        P(),
    )
    out_specs = (P("dp", "tensor", None), P("tensor", None, None, None))
    return jax.shard_map(
        on_device, mesh=mesh, in_specs=in_specs, out_specs=out_specs, check_vma=False
    )
```

```python
import functools

import jax
import jax.numpy as jnp
from jax import lax
from jax.experimental import pallas as pl
from jax.experimental.pallas import tpu as pltpu
from jax.sharding import PartitionSpec as P

MESH = pl.DeviceIdType.MESH
BLK = 128
CHUNK = 512
KEPT = 12
GRID_Y = 8
F32 = jnp.float32
BF16 = jnp.bfloat16


def kernel(
    cfg,
    attn_hbm, cot_hbm, res_hbm, lo_hbm, lc_hbm, ko_hbm, kc_hbm, bounds_hbm,
    new_hbm, kept_hbm,
    lo_ref, lc_ref, ko_ref, kc_ref, bounds_ref,
    attn_v, own_v, res_v, new_v, at_own, at_pair, at_far, pair, far, acc,
    rho, kappa, hit, idx_v, idx_s,
    contrib, partner_in, share, gathered, totals,
    small_sem, load_sem, idx_sem, store_sem, ring_send, ring_recv,
    word, pair_send, pair_recv, rs_send, rs_extra, rs_recv, ag_send, ag_recv, swap_send, swap_recv,
):
    chips, n_z = cfg["chips"], cfg["n_z"]
    half = chips // 2
    n_pair = n_z // 2 - 1
    rows = attn_hbm.shape[1]
    width = cot_hbm.shape[1]
    tokens = cot_hbm.shape[0]
    quarters = width // CHUNK
    per_chunk = CHUNK // BLK
    n_cols = width // BLK
    regions = 2 * chips
    magic = -(-(1 << 20) // n_cols)
    tiles = regions * KEPT // 8
    own_tiles = tiles // chips
    half_tiles = tiles // 2

    dp = lax.axis_index("dp")
    z = lax.axis_index("tensor")
    chip = dp // 2
    core = lax.rem(dp, 2)
    right = lax.rem(z + 1, n_z)
    left = lax.rem(z + n_z - 1, n_z)
    partner = dp + 1 - 2 * core
    lane_row = lax.rem(chip, half)
    owner = chip // half == core
    n_x, n_y = cfg["n_x"], cfg["n_y"]
    x, y = chip // n_y, lax.rem(chip, n_y)
    near_x = [lax.rem(x + step, n_x) * n_y + y for step in sorted({1, n_x - 1}) if n_x > 1]
    near_y = [x * n_y + lax.rem(y + step, n_y) for step in sorted({1, n_y - 1}) if n_y > 1]

    stages = [near_x] * max(n_x // 2 - 1, 0) + [near_y] * (n_y // 2)

    def pass_word(stage):
        if 0 < stage <= len(stages):
            pl.semaphore_wait(word.at[stage - 1], len(stages[stage - 1]))
        if stage < len(stages):
            tell(word.at[stage], stages[stage])


    loads = [
        pltpu.make_async_copy(attn_hbm, attn_v, load_sem.at[0]),
    ]
    for q in range(quarters):
        cols = pl.ds(q * CHUNK, CHUNK)
        loads.append(pltpu.make_async_copy(cot_hbm.at[:, cols], own_v.at[q], load_sem.at[1 + q]))
        loads.append(
            pltpu.make_async_copy(res_hbm.at[:, cols], res_v.at[q], load_sem.at[1 + quarters + q])
        )
    small = [
        pltpu.make_async_copy(a, b, small_sem.at[i])
        for i, (a, b) in enumerate(
            (
                (lo_hbm, lo_ref),
                (lc_hbm, lc_ref),
                (ko_hbm, ko_ref),
                (kc_hbm, kc_ref),
                (bounds_hbm, bounds_ref),
            )
        )
    ]
    for copy in small + loads:
        copy.start()

    barrier = pltpu.get_barrier_semaphore()
    for to in (left, right):
        pl.semaphore_signal(
            barrier, inc=1, device_id={"dp": dp, "tensor": to}, device_id_type=MESH
        )
    pl.semaphore_signal(
        barrier, inc=1, device_id={"dp": partner, "tensor": z}, device_id_type=MESH
    )

    def tell(sem, near):
        for to in near:
            pl.semaphore_signal(
                sem, inc=1, device_id={"dp": 2 * to + core, "tensor": z}, device_id_type=MESH
            )

    tell(barrier, near_x + near_y)
    pl.semaphore_wait(barrier, 3 + len(near_x) + len(near_y))

    def hop(side, step, q):
        to = right if side == 0 else left
        if step == 1:
            src = cot_hbm.at[:, pl.ds(pl.multiple_of(q * CHUNK, CHUNK), CHUNK)]
        elif step <= n_pair:
            src = pair.at[step - 2, q, pl.ds(side * tokens, tokens)]
        else:
            src = pair.at[
                step - 2, q, pl.ds(side * tokens + side * (tokens // 2), tokens // 2)
            ]
        if step <= n_pair:
            dst = pair.at[step - 1, q, pl.ds(side * tokens, tokens)]
        else:
            dst = far.at[q, pl.ds(side * (tokens // 2), tokens // 2)]
        return pltpu.make_async_remote_copy(
            src_ref=src,
            dst_ref=dst,
            send_sem=ring_send.at[side, step - 1, q],
            recv_sem=ring_recv.at[side, step - 1, q],
            device_id={"dp": dp, "tensor": to},
            device_id_type=MESH,
        )

    def first(q, carry):
        hop(0, 1, q).start()
        hop(1, 1, q).start()
        return carry

    lax.fori_loop(0, quarters, first, 0)

    pass_word(0)

    for copy in small:
        copy.wait()
    offsets = lo_ref[...]
    live = lax.broadcasted_iota(jnp.int32, offsets.shape, 0) < lc_ref[...]
    starts = bounds_ref[:, 0:regions]
    where_abs = starts + offsets
    where_row = (where_abs * magic) >> 20
    where_col = where_abs - where_row * n_cols
    rho[...] = jnp.full(rho.shape, -1, jnp.int32)
    kappa[...] = jnp.full(kappa.shape, -1, jnp.int32)
    rho[0:regions, 0 : offsets.shape[0]] = jnp.where(live, where_row, -1).T
    kappa[0:regions, 0 : offsets.shape[0]] = where_col.T
    hit[...] = jnp.zeros(hit.shape, F32)

    sent = jnp.where(live, offsets, -1)
    idx_v[...] = jnp.zeros(idx_v.shape, jnp.int32)
    nowhere = rows * n_cols
    for j in range(KEPT):
        wanted = ko_ref[j]
        same = jnp.where(sent == wanted, 1, 0)
        found = jnp.sum(same, axis=0, keepdims=True) * jnp.where(j < kc_ref[...], 1, 0)
        kept_abs = starts + wanted
        kept_row = (kept_abs * magic) >> 20
        position = (kept_abs - kept_row * n_cols) * rows + kept_row
        idx_v[j : j + 1, 0:regions] = jnp.where(found > 0, position, nowhere)
    acc[nowhere : nowhere + 8, :] = jnp.zeros((8, BLK), F32)

    pass_word(1)

    loads[0].wait()

    def turned(source):
        start = pl.multiple_of(source * tokens, tokens)
        return attn_v[pl.ds(start, tokens), :].astype(F32).T.astype(BF16)

    at_own[...] = turned(z)
    index_copy = pltpu.make_async_copy(idx_v, idx_s, idx_sem)
    index_copy.start()

    def accumulate(q, lhs, rhs_ref, start):
        for part in range(CHUNK // 256):
            got = jnp.dot(
                lhs, rhs_ref[:, part * 256 : part * 256 + 256], preferred_element_type=F32
            )
            for b in range(2):
                place = pl.ds(
                    pl.multiple_of((q * per_chunk + part * 2 + b) * rows, rows), rows
                )
                block = got[:, b * BLK : b * BLK + BLK]
                if start is None:
                    acc[place, :] = acc[place, :] + block
                else:
                    col = (part * 2 + b) * BLK
                    acc[place, :] = start[:, col : col + BLK].astype(F32) + block

    for copy in loads[1:]:
        copy.wait()

    def own_step(q, carry):
        accumulate(q, at_own[...], own_v.at[q], res_v.at[q])
        return carry

    lax.fori_loop(0, quarters, own_step, 0)
    pass_word(2)
    for d in range(1, n_pair + 1):
        at_pair[d - 1, :, 0:tokens] = turned(lax.rem(z + n_z - d, n_z))
        at_pair[d - 1, :, tokens : 2 * tokens] = turned(lax.rem(z + d, n_z))
    at_far[...] = turned(lax.rem(z + n_z // 2, n_z))

    mask_loops = range(2, n_pair + 1) if n_pair > 1 else range(1, n_pair + 1)
    per_visit = -(-regions // (quarters * len(mask_loops)))
    row_of = lax.broadcasted_iota(jnp.int32, (rows, BLK), 0)
    col_of = lax.broadcasted_iota(jnp.int32, (BLK, BLK), 0)

    def mark(visit):
        total = hit[...]
        for i in range(per_visit):
            r = visit * per_visit + i
            in_row = jnp.where(row_of == rho[pl.ds(r, 1), :], 1.0, 0.0).astype(BF16)
            in_col = jnp.where(col_of == kappa[pl.ds(r, 1), :], 1.0, 0.0).astype(BF16)
            total = total + lax.dot_general(
                in_row, in_col, (((1,), (1,)), ((), ())), preferred_element_type=F32
            )
        hit[...] = total

    for d in range(1, n_pair + 1):

        def pair_step(q, carry, d=d):
            hop(0, d, q).wait_recv()
            hop(0, d + 1, q).start()
            hop(1, d, q).wait_recv()
            hop(1, d + 1, q).start()
            accumulate(q, at_pair[d - 1], pair.at[d - 1, q], None)
            if d in mask_loops:
                mark((d - mask_loops[0]) * quarters + q)
            return carry

        pass_word(d + 2)
        lax.fori_loop(0, quarters, pair_step, 0)

    def far_step(q, carry):
        hop(0, n_pair + 1, q).wait_recv()
        hop(1, n_pair + 1, q).wait_recv()
        accumulate(q, at_far[...], far.at[q], None)
        return carry

    for stage in range(n_pair + 3, len(stages) + 1):
        pass_word(stage)
    index_copy.wait()
    lax.fori_loop(0, quarters, far_step, 0)

    def pick_from(base):
        def pick(piece, carry):
            got = []
            for i in range(own_tiles):
                begin = (base + piece * own_tiles + i) * 8
                j = begin // regions
                for m in range(8):
                    at = idx_s[j, begin - j * regions + m]
                    at = jnp.minimum(jnp.maximum(at, 0), nowhere)
                    got.append(acc[pl.ds(at, 1), :])
            for i in range(own_tiles):
                for m in range(8):
                    contrib[base + piece * own_tiles + i, m : m + 1, :] = got[8 * i + m]
            return carry

        lax.fori_loop(0, half, pick, 0)

    mine = core * half_tiles
    theirs = (1 - core) * half_tiles
    pick_from(theirs)
    to_partner = pltpu.make_async_remote_copy(
        src_ref=contrib.at[pl.ds(theirs, half_tiles)],
        dst_ref=partner_in,
        send_sem=pair_send,
        recv_sem=pair_recv,
        device_id={"dp": partner, "tensor": z},
        device_id_type=MESH,
    )
    to_partner.start()
    pick_from(mine)
    to_partner.wait_recv()
    share[...] = contrib[pl.ds(mine, half_tiles)] + partner_in[...]

    def scatter(j, send_sem):
        slot = lax.rem(lane_row + j, half)
        return pltpu.make_async_remote_copy(
            src_ref=share.at[pl.ds(slot * own_tiles, own_tiles)],
            dst_ref=gathered.at[chip],
            send_sem=send_sem,
            recv_sem=rs_recv,
            device_id={"dp": 2 * (core * half + slot) + core, "tensor": z},
            device_id_type=MESH,
        )

    def scatter_step(j, carry):
        scatter(j, rs_send).start()
        return carry

    @pl.when(jnp.logical_not(owner))
    def _():
        scatter(0, rs_extra).start()

    lax.fori_loop(1, half, scatter_step, 0)

    for c in range(n_cols):
        keep = hit[:, c : c + 1] < 0.5
        value = acc[c * rows : (c + 1) * rows, :]
        new_v[:, c * BLK : (c + 1) * BLK] = jnp.where(keep, value, 0.0).astype(BF16)
    write = pltpu.make_async_copy(new_v, new_hbm, store_sem)
    write.start()

    def hand_out(j):
        return pltpu.make_async_remote_copy(
            src_ref=totals.at[pl.ds(chip * own_tiles, own_tiles)],
            dst_ref=totals.at[pl.ds(chip * own_tiles, own_tiles)],
            send_sem=ag_send,
            recv_sem=ag_recv,
            device_id={"dp": 2 * lax.rem(chip + j, chips) + core, "tensor": z},
            device_id_type=MESH,
        )

    def hand_step(j, carry):
        hand_out(j).start()
        return carry

    def wait_for(ref, count, sem):
        if count == 0:
            return
        part = ref.at[pl.ds(0, count)]
        pltpu.make_async_copy(part, part, sem).wait()

    @pl.when(owner)
    def _():
        gathered[chip] = share[pl.ds(lane_row * own_tiles, own_tiles)]
        wait_for(gathered, chips - 1, rs_recv)
        total = gathered[0]
        for k in range(1, chips):
            total = total + gathered[k]
        totals[pl.ds(chip * own_tiles, own_tiles)] = total
        lax.fori_loop(1, chips, hand_step, 0)
        wait_for(totals, (half - 1) * own_tiles, ag_recv)

    @pl.when(jnp.logical_not(owner))
    def _():
        wait_for(totals, half_tiles, ag_recv)

    swap = pltpu.make_async_remote_copy(
        src_ref=totals.at[pl.ds(mine, half_tiles)],
        dst_ref=totals.at[pl.ds(mine, half_tiles)],
        send_sem=swap_send,
        recv_sem=swap_recv,
        device_id={"dp": partner, "tensor": z},
        device_id_type=MESH,
    )
    swap.start()

    for d in range(1, n_pair + 2):

        def sent_step(q, carry, d=d):
            hop(0, d, q).wait_send()
            hop(1, d, q).wait_send()
            return carry

        lax.fori_loop(0, quarters, sent_step, 0)
    to_partner.wait_send()
    wait_for(share, (half - 1) * own_tiles, rs_send)

    @pl.when(jnp.logical_not(owner))
    def _():
        scatter(0, rs_extra).wait_send()

    @pl.when(owner)
    def _():
        wait_for(totals, (chips - 1) * own_tiles, ag_send)

    write.wait()
    swap.wait()
    keep_out = pltpu.make_async_copy(totals, kept_hbm, store_sem)
    keep_out.start()
    keep_out.wait()


def finish(new_ref, kept_ref, new_out, kept_out, new_v, kept_v, sem_in, sem_out):
    pieces = new_v.shape[0]
    each = new_ref.shape[0] // pieces
    moves = [(kept_ref, kept_v, kept_out)]
    for i in range(pieces):
        part = pl.ds(i * each, each)
        moves.append((new_ref.at[part], new_v.at[i], new_out.at[part]))
    inward = [
        pltpu.make_async_copy(a, b, sem_in.at[i]) for i, (a, b, _) in enumerate(moves)
    ]
    outward = [
        pltpu.make_async_copy(b, c, sem_out.at[i]) for i, (_, b, c) in enumerate(moves)
    ]
    for copy in inward:
        copy.start()
    for got, put in zip(inward, outward):
        got.wait()
        put.start()
    for put in outward:
        put.wait()


def on_device(
    attn_out, cotangent, residual, local_offsets, local_counts, kept_offsets, kept_counts, bounds
):
    n_dp, n_z = lax.axis_size("dp"), lax.axis_size("tensor")
    chips = n_dp // 2
    n_y = GRID_Y if chips % GRID_Y == 0 else chips
    n_x = chips // n_y
    tokens, width = cotangent.shape
    rows = attn_out.shape[1]
    regions = local_offsets.shape[2]
    n_pair = n_z // 2 - 1
    quarters = width // CHUNK
    n_cols = width // BLK
    padded = -(-regions // 8) * 8 + 8 * quarters
    anywhere = pl.BlockSpec(memory_space=pl.ANY)
    slots = local_offsets.shape[3]
    dma = pltpu.SemaphoreType.DMA
    tiles = regions * KEPT // 8
    new, kept = pl.pallas_call(
        functools.partial(kernel, {"chips": chips, "n_z": n_z, "n_x": n_x, "n_y": n_y}),
        out_shape=(
            jax.ShapeDtypeStruct((rows, width), BF16),
            jax.ShapeDtypeStruct((tiles, 8, BLK), F32),
        ),
        in_specs=[anywhere] * 8,
        out_specs=(anywhere, anywhere),
        scratch_shapes=[
            pltpu.VMEM((slots, regions), jnp.int32),
            pltpu.VMEM((1, regions), jnp.int32),
            pltpu.VMEM((KEPT, 1, regions), jnp.int32),
            pltpu.VMEM((1, regions), jnp.int32),
            pltpu.VMEM((1, regions + 1), jnp.int32),
            pltpu.VMEM(attn_out.shape, BF16),
            pltpu.VMEM((quarters, tokens, CHUNK), BF16),
            pltpu.VMEM((quarters, rows, CHUNK), BF16),
            pltpu.VMEM((rows, width), BF16),
            pltpu.VMEM((rows, tokens), BF16),
            pltpu.VMEM((n_pair, rows, 2 * tokens), BF16),
            pltpu.VMEM((rows, tokens), BF16),
            pltpu.VMEM((n_pair, quarters, 2 * tokens, CHUNK), BF16),
            pltpu.VMEM((quarters, tokens, CHUNK), BF16),
            pltpu.VMEM((rows * n_cols + 8, BLK), F32),
            pltpu.VMEM((padded, BLK), jnp.int32),
            pltpu.VMEM((padded, BLK), jnp.int32),
            pltpu.VMEM((rows, BLK), F32),
            pltpu.VMEM((16, BLK), jnp.int32),
            pltpu.SMEM((16, BLK), jnp.int32),
            pltpu.VMEM((tiles, 8, BLK), F32),
            pltpu.VMEM((tiles // 2, 8, BLK), F32),
            pltpu.VMEM((tiles // 2, 8, BLK), F32),
            pltpu.VMEM((chips, tiles // chips, 8, BLK), F32),
            pltpu.VMEM((tiles, 8, BLK), F32),
            dma((5,)),
            dma((1 + 2 * quarters,)),
            dma,
            dma,
            dma((2, n_pair + 1, quarters)),
            dma((2, n_pair + 1, quarters)),
            pltpu.SemaphoreType.REGULAR((n_x + n_y,)),
            dma,
            dma,
            dma,
            dma,
            dma,
            dma,
            dma,
            dma,
            dma,
        ],
        compiler_params=pltpu.CompilerParams(collective_id=0, has_side_effects=True),
    )(
        attn_out,
        cotangent,
        residual[0],
        local_offsets[0, 0].T,
        local_counts[0],
        kept_offsets.transpose(2, 0, 1),
        kept_counts,
        bounds[None],
    )
    pieces = 4
    new, kept = pl.pallas_call(
        finish,
        out_shape=(
            jax.ShapeDtypeStruct(new.shape, BF16),
            jax.ShapeDtypeStruct(kept.shape, F32),
        ),
        in_specs=[anywhere] * 2,
        out_specs=(anywhere, anywhere),
        scratch_shapes=[
            pltpu.VMEM((pieces, rows // pieces, width), BF16),
            pltpu.VMEM(kept.shape, F32),
            dma((pieces + 1,)),
            dma((pieces + 1,)),
        ],
    )(new, kept)
    return new[None], kept.reshape(KEPT, regions, BLK).transpose(1, 0, 2)[None]


def solution(mesh):
    in_specs = (
        P("dp", "tensor"),
        P(("dp", "tensor"), None),
        P("dp", "tensor", None),
        P("dp", "tensor", None, None),
        P("dp", "tensor", None),
        P("tensor", None, None),
        P("tensor", None),
        P(),
    )
    out_specs = (P("dp", "tensor", None), P("tensor", None, None, None))
    return jax.shard_map(
        on_device, mesh=mesh, in_specs=in_specs, out_specs=out_specs, check_vma=False
    )
```

```python
import functools

import jax
import jax.numpy as jnp
from jax import lax
from jax.experimental import pallas as pl
from jax.experimental.pallas import tpu as pltpu
from jax.sharding import PartitionSpec as P

MESH = pl.DeviceIdType.MESH
BLK = 128
CHUNK = 512
KEPT = 12
GRID_Y = 8
F32 = jnp.float32
BF16 = jnp.bfloat16


def kernel(
    cfg,
    attn_hbm, cot_hbm, res_hbm, lo_hbm, lc_hbm, ko_hbm, kc_hbm, bounds_hbm,
    new_hbm, kept_hbm,
    lo_ref, lc_ref, ko_ref, kc_ref, bounds_ref,
    attn_v, own_v, res_v, new_v, at_own, at_pair, at_far, pair, far, acc,
    rho, kappa, hit, idx_v, idx_s,
    contrib, partner_in, share, gathered, totals,
    small_sem, load_sem, idx_sem, store_sem, ring_send, ring_recv,
    word, pair_send, pair_recv, rs_send, rs_recv, ag_send, ag_recv, swap_send, swap_recv,
):
    chips, n_z = cfg["chips"], cfg["n_z"]
    half = chips // 2
    n_pair = n_z // 2 - 1
    rows = attn_hbm.shape[1]
    width = cot_hbm.shape[1]
    tokens = cot_hbm.shape[0]
    quarters = width // CHUNK
    per_chunk = CHUNK // BLK
    n_cols = width // BLK
    regions = 2 * chips
    magic = -(-(1 << 20) // n_cols)
    tiles = regions * KEPT // 8
    own_tiles = tiles // chips
    half_tiles = tiles // 2

    dp = lax.axis_index("dp")
    z = lax.axis_index("tensor")
    chip = dp // 2
    core = lax.rem(dp, 2)
    right = lax.rem(z + 1, n_z)
    left = lax.rem(z + n_z - 1, n_z)
    partner = dp + 1 - 2 * core
    lane_row = lax.rem(chip, half)
    owner = chip // half == core
    n_x, n_y = cfg["n_x"], cfg["n_y"]
    x, y = chip // n_y, lax.rem(chip, n_y)
    near_x = [lax.rem(x + step, n_x) * n_y + y for step in sorted({1, n_x - 1}) if n_x > 1]
    near_y = [x * n_y + lax.rem(y + step, n_y) for step in sorted({1, n_y - 1}) if n_y > 1]

    stages = [near_x] * max(n_x // 2 - 1, 0) + [near_y] * (n_y // 2)

    def pass_word(stage):
        if 0 < stage <= len(stages):
            pl.semaphore_wait(word.at[stage - 1], len(stages[stage - 1]))
        if stage < len(stages):
            tell(word.at[stage], stages[stage])


    loads = [
        pltpu.make_async_copy(attn_hbm, attn_v, load_sem.at[0]),
    ]
    for q in range(quarters):
        cols = pl.ds(q * CHUNK, CHUNK)
        loads.append(pltpu.make_async_copy(cot_hbm.at[:, cols], own_v.at[q], load_sem.at[1 + q]))
        loads.append(
            pltpu.make_async_copy(res_hbm.at[:, cols], res_v.at[q], load_sem.at[1 + quarters + q])
        )
    small = [
        pltpu.make_async_copy(a, b, small_sem.at[i])
        for i, (a, b) in enumerate(
            (
                (lo_hbm, lo_ref),
                (lc_hbm, lc_ref),
                (ko_hbm, ko_ref),
                (kc_hbm, kc_ref),
                (bounds_hbm, bounds_ref),
            )
        )
    ]
    for copy in small + loads:
        copy.start()

    barrier = pltpu.get_barrier_semaphore()
    for to in (left, right):
        pl.semaphore_signal(
            barrier, inc=1, device_id={"dp": dp, "tensor": to}, device_id_type=MESH
        )
    pl.semaphore_signal(
        barrier, inc=1, device_id={"dp": partner, "tensor": z}, device_id_type=MESH
    )

    def tell(sem, near):
        for to in near:
            pl.semaphore_signal(
                sem, inc=1, device_id={"dp": 2 * to + core, "tensor": z}, device_id_type=MESH
            )

    tell(barrier, near_x + near_y)
    pl.semaphore_wait(barrier, 3 + len(near_x) + len(near_y))

    def hop(side, step, q):
        to = right if side == 0 else left
        if step == 1:
            src = cot_hbm.at[:, pl.ds(pl.multiple_of(q * CHUNK, CHUNK), CHUNK)]
        elif step <= n_pair:
            src = pair.at[step - 2, q, pl.ds(side * tokens, tokens)]
        else:
            src = pair.at[
                step - 2, q, pl.ds(side * tokens + side * (tokens // 2), tokens // 2)
            ]
        if step <= n_pair:
            dst = pair.at[step - 1, q, pl.ds(side * tokens, tokens)]
        else:
            dst = far.at[q, pl.ds(side * (tokens // 2), tokens // 2)]
        return pltpu.make_async_remote_copy(
            src_ref=src,
            dst_ref=dst,
            send_sem=ring_send.at[side, step - 1, q],
            recv_sem=ring_recv.at[side, step - 1, q],
            device_id={"dp": dp, "tensor": to},
            device_id_type=MESH,
        )

    def first(q, carry):
        hop(0, 1, q).start()
        hop(1, 1, q).start()
        return carry

    lax.fori_loop(0, quarters, first, 0)

    pass_word(0)

    for copy in small:
        copy.wait()
    offsets = lo_ref[...]
    live = lax.broadcasted_iota(jnp.int32, offsets.shape, 0) < lc_ref[...]
    starts = bounds_ref[:, 0:regions]
    where_abs = starts + offsets
    where_row = (where_abs * magic) >> 20
    where_col = where_abs - where_row * n_cols
    rho[...] = jnp.full(rho.shape, -1, jnp.int32)
    kappa[...] = jnp.full(kappa.shape, -1, jnp.int32)
    rho[0:regions, 0 : offsets.shape[0]] = jnp.where(live, where_row, -1).T
    kappa[0:regions, 0 : offsets.shape[0]] = where_col.T
    hit[...] = jnp.zeros(hit.shape, F32)

    sent = jnp.where(live, offsets, -1)
    idx_v[...] = jnp.zeros(idx_v.shape, jnp.int32)
    nowhere = rows * n_cols
    for j in range(KEPT):
        wanted = ko_ref[j]
        same = jnp.where(sent == wanted, 1, 0)
        found = jnp.sum(same, axis=0, keepdims=True) * jnp.where(j < kc_ref[...], 1, 0)
        kept_abs = starts + wanted
        kept_row = (kept_abs * magic) >> 20
        position = (kept_abs - kept_row * n_cols) * rows + kept_row
        idx_v[j : j + 1, 0:regions] = jnp.where(found > 0, position, nowhere)
    acc[nowhere : nowhere + 8, :] = jnp.zeros((8, BLK), F32)

    pass_word(1)

    loads[0].wait()

    def turned(source):
        start = pl.multiple_of(source * tokens, tokens)
        return attn_v[pl.ds(start, tokens), :].astype(F32).T.astype(BF16)

    at_own[...] = turned(z)
    index_copy = pltpu.make_async_copy(idx_v, idx_s, idx_sem)
    index_copy.start()

    def accumulate(q, lhs, rhs_ref, start):
        for part in range(CHUNK // 256):
            got = jnp.dot(
                lhs, rhs_ref[:, part * 256 : part * 256 + 256], preferred_element_type=F32
            )
            for b in range(2):
                place = pl.ds(
                    pl.multiple_of((q * per_chunk + part * 2 + b) * rows, rows), rows
                )
                block = got[:, b * BLK : b * BLK + BLK]
                if start is None:
                    acc[place, :] = acc[place, :] + block
                else:
                    col = (part * 2 + b) * BLK
                    acc[place, :] = start[:, col : col + BLK].astype(F32) + block

    for copy in loads[1:]:
        copy.wait()

    def own_step(q, carry):
        accumulate(q, at_own[...], own_v.at[q], res_v.at[q])
        return carry

    lax.fori_loop(0, quarters, own_step, 0)
    pass_word(2)
    for d in range(1, n_pair + 1):
        at_pair[d - 1, :, 0:tokens] = turned(lax.rem(z + n_z - d, n_z))
        at_pair[d - 1, :, tokens : 2 * tokens] = turned(lax.rem(z + d, n_z))
    at_far[...] = turned(lax.rem(z + n_z // 2, n_z))

    mask_loops = range(2, n_pair + 1) if n_pair > 1 else range(1, n_pair + 1)
    per_visit = -(-regions // (quarters * len(mask_loops)))
    row_of = lax.broadcasted_iota(jnp.int32, (rows, BLK), 0)
    col_of = lax.broadcasted_iota(jnp.int32, (BLK, BLK), 0)

    def mark(visit):
        total = hit[...]
        for i in range(per_visit):
            r = visit * per_visit + i
            in_row = jnp.where(row_of == rho[pl.ds(r, 1), :], 1.0, 0.0).astype(BF16)
            in_col = jnp.where(col_of == kappa[pl.ds(r, 1), :], 1.0, 0.0).astype(BF16)
            total = total + lax.dot_general(
                in_row, in_col, (((1,), (1,)), ((), ())), preferred_element_type=F32
            )
        hit[...] = total

    for d in range(1, n_pair + 1):

        def pair_step(q, carry, d=d):
            hop(0, d, q).wait_recv()
            hop(0, d + 1, q).start()
            hop(1, d, q).wait_recv()
            hop(1, d + 1, q).start()
            accumulate(q, at_pair[d - 1], pair.at[d - 1, q], None)
            if d in mask_loops:
                mark((d - mask_loops[0]) * quarters + q)
            return carry

        pass_word(d + 2)
        lax.fori_loop(0, quarters, pair_step, 0)

    def far_step(q, carry):
        hop(0, n_pair + 1, q).wait_recv()
        hop(1, n_pair + 1, q).wait_recv()
        accumulate(q, at_far[...], far.at[q], None)
        return carry

    for stage in range(n_pair + 3, len(stages) + 1):
        pass_word(stage)
    index_copy.wait()
    lax.fori_loop(0, quarters, far_step, 0)

    def far_first(k, n_rows, n_along):
        step = k // n_rows
        aside = (step + 1) // 2
        along = n_along // 2 + aside - 2 * aside * lax.rem(step, 2)
        return along + n_along * (n_rows - 1 - lax.rem(k, n_rows))

    half_rows = max(half // n_y, 1)

    def slot_of(k):
        return lax.rem(lane_row + far_first(k, half_rows, half // half_rows), half)

    def pick(base):
        got = []
        for i in range(own_tiles):
            begin = (base + i) * 8
            j = begin // regions
            for m in range(8):
                at = idx_s[j, begin - j * regions + m]
                at = jnp.minimum(jnp.maximum(at, 0), nowhere)
                got.append(acc[pl.ds(at, 1), :])
        for i in range(own_tiles):
            for m in range(8):
                contrib[base + i, m : m + 1, :] = got[8 * i + m]

    mine = core * half_tiles
    theirs = (1 - core) * half_tiles

    def to_partner(k):
        at = slot_of(k) * own_tiles
        return pltpu.make_async_remote_copy(
            src_ref=contrib.at[pl.ds(theirs + at, own_tiles)],
            dst_ref=partner_in.at[pl.ds(at, own_tiles)],
            send_sem=pair_send.at[k],
            recv_sem=pair_recv.at[k],
            device_id={"dp": partner, "tensor": z},
            device_id_type=MESH,
        )

    def scatter(k):
        slot = slot_of(k)
        return pltpu.make_async_remote_copy(
            src_ref=share.at[pl.ds(slot * own_tiles, own_tiles)],
            dst_ref=gathered.at[chip],
            send_sem=rs_send.at[k],
            recv_sem=rs_recv,
            device_id={"dp": 2 * (core * half + slot) + core, "tensor": z},
            device_id_type=MESH,
        )

    def partner_step(k, carry):
        pick(theirs + slot_of(k) * own_tiles)
        to_partner(k).start()
        return carry

    def share_piece(k):
        at = slot_of(k) * own_tiles
        pick(mine + at)
        to_partner(k).wait_recv()
        piece = pl.ds(at, own_tiles)
        share[piece] = contrib[pl.ds(mine + at, own_tiles)] + partner_in[piece]

    def scatter_step(k, carry):
        share_piece(k)
        scatter(k).start()
        return carry

    lax.fori_loop(0, half, partner_step, 0)
    lax.fori_loop(0, half - 1, scatter_step, 0)
    share_piece(half - 1)

    @pl.when(jnp.logical_not(owner))
    def _():
        scatter(half - 1).start()

    for c in range(n_cols):
        keep = hit[:, c : c + 1] < 0.5
        value = acc[c * rows : (c + 1) * rows, :]
        new_v[:, c * BLK : (c + 1) * BLK] = jnp.where(keep, value, 0.0).astype(BF16)
    write = pltpu.make_async_copy(new_v, new_hbm, store_sem)
    write.start()

    def hand_out(k):
        return pltpu.make_async_remote_copy(
            src_ref=totals.at[pl.ds(chip * own_tiles, own_tiles)],
            dst_ref=totals.at[pl.ds(chip * own_tiles, own_tiles)],
            send_sem=ag_send,
            recv_sem=ag_recv,
            device_id={"dp": 2 * lax.rem(chip + far_first(k, n_x, n_y), chips) + core, "tensor": z},
            device_id_type=MESH,
        )

    def hand_step(k, carry):
        hand_out(k).start()
        return carry

    def wait_for(ref, count, sem):
        if count == 0:
            return
        part = ref.at[pl.ds(0, count)]
        pltpu.make_async_copy(part, part, sem).wait()

    @pl.when(owner)
    def _():
        gathered[chip] = share[pl.ds(lane_row * own_tiles, own_tiles)]
        wait_for(gathered, chips - 1, rs_recv)
        total = gathered[0]
        for k in range(1, chips):
            total = total + gathered[k]
        totals[pl.ds(chip * own_tiles, own_tiles)] = total
        lax.fori_loop(0, chips - 1, hand_step, 0)
        wait_for(totals, (half - 1) * own_tiles, ag_recv)

    @pl.when(jnp.logical_not(owner))
    def _():
        wait_for(totals, half_tiles, ag_recv)

    swap = pltpu.make_async_remote_copy(
        src_ref=totals.at[pl.ds(mine, half_tiles)],
        dst_ref=totals.at[pl.ds(mine, half_tiles)],
        send_sem=swap_send,
        recv_sem=swap_recv,
        device_id={"dp": partner, "tensor": z},
        device_id_type=MESH,
    )
    swap.start()

    for d in range(1, n_pair + 2):

        def sent_step(q, carry, d=d):
            hop(0, d, q).wait_send()
            hop(1, d, q).wait_send()
            return carry

        lax.fori_loop(0, quarters, sent_step, 0)

    def left_step(k, carry):
        to_partner(k).wait_send()
        return carry

    def scattered_step(k, carry):
        scatter(k).wait_send()
        return carry

    lax.fori_loop(0, half, left_step, 0)
    lax.fori_loop(0, half - 1, scattered_step, 0)

    @pl.when(jnp.logical_not(owner))
    def _():
        scatter(half - 1).wait_send()

    @pl.when(owner)
    def _():
        wait_for(totals, (chips - 1) * own_tiles, ag_send)

    write.wait()
    swap.wait()
    keep_out = pltpu.make_async_copy(totals, kept_hbm, store_sem)
    keep_out.start()
    keep_out.wait()


def finish(new_ref, kept_ref, new_out, kept_out, new_v, kept_v, sem_in, sem_out):
    pieces = new_v.shape[0]
    each = new_ref.shape[0] // pieces
    moves = [(kept_ref, kept_v, kept_out)]
    for i in range(pieces):
        part = pl.ds(i * each, each)
        moves.append((new_ref.at[part], new_v.at[i], new_out.at[part]))
    inward = [
        pltpu.make_async_copy(a, b, sem_in.at[i]) for i, (a, b, _) in enumerate(moves)
    ]
    outward = [
        pltpu.make_async_copy(b, c, sem_out.at[i]) for i, (_, b, c) in enumerate(moves)
    ]
    for copy in inward:
        copy.start()
    for got, put in zip(inward, outward):
        got.wait()
        put.start()
    for put in outward:
        put.wait()


def on_device(
    attn_out, cotangent, residual, local_offsets, local_counts, kept_offsets, kept_counts, bounds
):
    n_dp, n_z = lax.axis_size("dp"), lax.axis_size("tensor")
    chips = n_dp // 2
    n_y = GRID_Y if chips % GRID_Y == 0 else chips
    n_x = chips // n_y
    tokens, width = cotangent.shape
    rows = attn_out.shape[1]
    regions = local_offsets.shape[2]
    n_pair = n_z // 2 - 1
    quarters = width // CHUNK
    n_cols = width // BLK
    padded = -(-regions // 8) * 8 + 8 * quarters
    anywhere = pl.BlockSpec(memory_space=pl.ANY)
    slots = local_offsets.shape[3]
    dma = pltpu.SemaphoreType.DMA
    tiles = regions * KEPT // 8
    new, kept = pl.pallas_call(
        functools.partial(kernel, {"chips": chips, "n_z": n_z, "n_x": n_x, "n_y": n_y}),
        out_shape=(
            jax.ShapeDtypeStruct((rows, width), BF16),
            jax.ShapeDtypeStruct((tiles, 8, BLK), F32),
        ),
        in_specs=[anywhere] * 8,
        out_specs=(anywhere, anywhere),
        scratch_shapes=[
            pltpu.VMEM((slots, regions), jnp.int32),
            pltpu.VMEM((1, regions), jnp.int32),
            pltpu.VMEM((KEPT, 1, regions), jnp.int32),
            pltpu.VMEM((1, regions), jnp.int32),
            pltpu.VMEM((1, regions + 1), jnp.int32),
            pltpu.VMEM(attn_out.shape, BF16),
            pltpu.VMEM((quarters, tokens, CHUNK), BF16),
            pltpu.VMEM((quarters, rows, CHUNK), BF16),
            pltpu.VMEM((rows, width), BF16),
            pltpu.VMEM((rows, tokens), BF16),
            pltpu.VMEM((n_pair, rows, 2 * tokens), BF16),
            pltpu.VMEM((rows, tokens), BF16),
            pltpu.VMEM((n_pair, quarters, 2 * tokens, CHUNK), BF16),
            pltpu.VMEM((quarters, tokens, CHUNK), BF16),
            pltpu.VMEM((rows * n_cols + 8, BLK), F32),
            pltpu.VMEM((padded, BLK), jnp.int32),
            pltpu.VMEM((padded, BLK), jnp.int32),
            pltpu.VMEM((rows, BLK), F32),
            pltpu.VMEM((16, BLK), jnp.int32),
            pltpu.SMEM((16, BLK), jnp.int32),
            pltpu.VMEM((tiles, 8, BLK), F32),
            pltpu.VMEM((tiles // 2, 8, BLK), F32),
            pltpu.VMEM((tiles // 2, 8, BLK), F32),
            pltpu.VMEM((chips, tiles // chips, 8, BLK), F32),
            pltpu.VMEM((tiles, 8, BLK), F32),
            dma((5,)),
            dma((1 + 2 * quarters,)),
            dma,
            dma,
            dma((2, n_pair + 1, quarters)),
            dma((2, n_pair + 1, quarters)),
            pltpu.SemaphoreType.REGULAR((n_x + n_y,)),
            dma((chips // 2,)),
            dma((chips // 2,)),
            dma((chips // 2,)),
            dma,
            dma,
            dma,
            dma,
            dma,
        ],
        compiler_params=pltpu.CompilerParams(collective_id=0, has_side_effects=True),
    )(
        attn_out,
        cotangent,
        residual[0],
        local_offsets[0, 0].T,
        local_counts[0],
        kept_offsets.transpose(2, 0, 1),
        kept_counts,
        bounds[None],
    )
    pieces = 4
    new, kept = pl.pallas_call(
        finish,
        out_shape=(
            jax.ShapeDtypeStruct(new.shape, BF16),
            jax.ShapeDtypeStruct(kept.shape, F32),
        ),
        in_specs=[anywhere] * 2,
        out_specs=(anywhere, anywhere),
        scratch_shapes=[
            pltpu.VMEM((pieces, rows // pieces, width), BF16),
            pltpu.VMEM(kept.shape, F32),
            dma((pieces + 1,)),
            dma((pieces + 1,)),
        ],
    )(new, kept)
    return new[None], kept.reshape(KEPT, regions, BLK).transpose(1, 0, 2)[None]


def solution(mesh):
    in_specs = (
        P("dp", "tensor"),
        P(("dp", "tensor"), None),
        P("dp", "tensor", None),
        P("dp", "tensor", None, None),
        P("dp", "tensor", None),
        P("tensor", None, None),
        P("tensor", None),
        P(),
    )
    out_specs = (P("dp", "tensor", None), P("tensor", None, None, None))
    return jax.shard_map(
        on_device, mesh=mesh, in_specs=in_specs, out_specs=out_specs, check_vma=False
    )
```

```python
import functools

import jax
import jax.numpy as jnp
from jax import lax
from jax.experimental import pallas as pl
from jax.experimental.pallas import tpu as pltpu
from jax.sharding import PartitionSpec as P

MESH = pl.DeviceIdType.MESH
BLK = 128
CHUNK = 512
KEPT = 12
GRID_Y = 8
F32 = jnp.float32
BF16 = jnp.bfloat16


def kernel(
    cfg,
    attn_hbm, cot_hbm, res_hbm, lo_hbm, lc_hbm, ko_hbm, kc_hbm, bounds_hbm,
    new_v, kept_ref,
    lo_ref, lc_ref, ko_ref, kc_ref, bounds_ref,
    attn_v, own_v, res_v, at_own, at_pair, at_far, pair, far, acc,
    rho, kappa, hit, idx_v, idx_s,
    contrib, partner_in, share, gathered, totals,
    small_sem, load_sem, idx_sem, ring_send, ring_recv,
    word, pair_send, pair_recv, rs_send, rs_recv, ag_send, ag_recv, swap_send, swap_recv,
):
    chips, n_z = cfg["chips"], cfg["n_z"]
    half = chips // 2
    n_pair = n_z // 2 - 1
    rows = attn_hbm.shape[1]
    width = cot_hbm.shape[1]
    tokens = cot_hbm.shape[0]
    quarters = width // CHUNK
    per_chunk = CHUNK // BLK
    n_cols = width // BLK
    regions = 2 * chips
    magic = -(-(1 << 20) // n_cols)
    tiles = regions * KEPT // 8
    own_tiles = tiles // chips
    half_tiles = tiles // 2

    dp = lax.axis_index("dp")
    z = lax.axis_index("tensor")
    chip = dp // 2
    core = lax.rem(dp, 2)
    right = lax.rem(z + 1, n_z)
    left = lax.rem(z + n_z - 1, n_z)
    partner = dp + 1 - 2 * core
    lane_row = lax.rem(chip, half)
    owner = chip // half == core
    n_x, n_y = cfg["n_x"], cfg["n_y"]
    x, y = chip // n_y, lax.rem(chip, n_y)
    near_x = [lax.rem(x + step, n_x) * n_y + y for step in sorted({1, n_x - 1}) if n_x > 1]
    near_y = [x * n_y + lax.rem(y + step, n_y) for step in sorted({1, n_y - 1}) if n_y > 1]

    stages = [near_x] * max(n_x // 2 - 1, 0) + [near_y] * (n_y // 2)

    def pass_word(stage):
        if 0 < stage <= len(stages):
            pl.semaphore_wait(word.at[stage - 1], len(stages[stage - 1]))
        if stage < len(stages):
            tell(word.at[stage], stages[stage])


    loads = [
        pltpu.make_async_copy(attn_hbm, attn_v, load_sem.at[0]),
    ]
    for q in range(quarters):
        cols = pl.ds(q * CHUNK, CHUNK)
        loads.append(pltpu.make_async_copy(cot_hbm.at[:, cols], own_v.at[q], load_sem.at[1 + q]))
        loads.append(
            pltpu.make_async_copy(res_hbm.at[:, cols], res_v.at[q], load_sem.at[1 + quarters + q])
        )
    small = [
        pltpu.make_async_copy(a, b, small_sem.at[i])
        for i, (a, b) in enumerate(
            (
                (lo_hbm, lo_ref),
                (lc_hbm, lc_ref),
                (ko_hbm, ko_ref),
                (kc_hbm, kc_ref),
                (bounds_hbm, bounds_ref),
            )
        )
    ]
    for copy in small + loads:
        copy.start()

    barrier = pltpu.get_barrier_semaphore()
    for to in (left, right):
        pl.semaphore_signal(
            barrier, inc=1, device_id={"dp": dp, "tensor": to}, device_id_type=MESH
        )
    pl.semaphore_signal(
        barrier, inc=1, device_id={"dp": partner, "tensor": z}, device_id_type=MESH
    )

    def tell(sem, near):
        for to in near:
            pl.semaphore_signal(
                sem, inc=1, device_id={"dp": 2 * to + core, "tensor": z}, device_id_type=MESH
            )

    tell(barrier, near_x + near_y)
    pl.semaphore_wait(barrier, 3 + len(near_x) + len(near_y))

    def hop(side, step, q):
        to = right if side == 0 else left
        if step == 1:
            src = cot_hbm.at[:, pl.ds(pl.multiple_of(q * CHUNK, CHUNK), CHUNK)]
        elif step <= n_pair:
            src = pair.at[step - 2, q, pl.ds(side * tokens, tokens)]
        else:
            src = pair.at[
                step - 2, q, pl.ds(side * tokens + side * (tokens // 2), tokens // 2)
            ]
        if step <= n_pair:
            dst = pair.at[step - 1, q, pl.ds(side * tokens, tokens)]
        else:
            dst = far.at[q, pl.ds(side * (tokens // 2), tokens // 2)]
        return pltpu.make_async_remote_copy(
            src_ref=src,
            dst_ref=dst,
            send_sem=ring_send.at[side, step - 1, q],
            recv_sem=ring_recv.at[side, step - 1, q],
            device_id={"dp": dp, "tensor": to},
            device_id_type=MESH,
        )

    def first(q, carry):
        hop(0, 1, q).start()
        hop(1, 1, q).start()
        return carry

    lax.fori_loop(0, quarters, first, 0)

    pass_word(0)

    for copy in small:
        copy.wait()
    offsets = lo_ref[...]
    live = lax.broadcasted_iota(jnp.int32, offsets.shape, 0) < lc_ref[...]
    starts = bounds_ref[:, 0:regions]
    where_abs = starts + offsets
    where_row = (where_abs * magic) >> 20
    where_col = where_abs - where_row * n_cols
    rho[...] = jnp.full(rho.shape, -1, jnp.int32)
    kappa[...] = jnp.full(kappa.shape, -1, jnp.int32)
    rho[0:regions, 0 : offsets.shape[0]] = jnp.where(live, where_row, -1).T
    kappa[0:regions, 0 : offsets.shape[0]] = where_col.T
    hit[...] = jnp.zeros(hit.shape, F32)

    sent = jnp.where(live, offsets, -1)
    idx_v[...] = jnp.zeros(idx_v.shape, jnp.int32)
    nowhere = rows * n_cols
    for j in range(KEPT):
        wanted = ko_ref[j]
        same = jnp.where(sent == wanted, 1, 0)
        found = jnp.sum(same, axis=0, keepdims=True) * jnp.where(j < kc_ref[...], 1, 0)
        kept_abs = starts + wanted
        kept_row = (kept_abs * magic) >> 20
        position = (kept_abs - kept_row * n_cols) * rows + kept_row
        idx_v[j : j + 1, 0:regions] = jnp.where(found > 0, position, nowhere)
    acc[nowhere : nowhere + 8, :] = jnp.zeros((8, BLK), F32)

    pass_word(1)

    loads[0].wait()

    def turned(source):
        start = pl.multiple_of(source * tokens, tokens)
        return attn_v[pl.ds(start, tokens), :].astype(F32).T.astype(BF16)

    at_own[...] = turned(z)
    index_copy = pltpu.make_async_copy(idx_v, idx_s, idx_sem)
    index_copy.start()

    def accumulate(q, lhs, rhs_ref, start):
        for part in range(CHUNK // 256):
            got = jnp.dot(
                lhs, rhs_ref[:, part * 256 : part * 256 + 256], preferred_element_type=F32
            )
            for b in range(2):
                place = pl.ds(
                    pl.multiple_of((q * per_chunk + part * 2 + b) * rows, rows), rows
                )
                block = got[:, b * BLK : b * BLK + BLK]
                if start is None:
                    acc[place, :] = acc[place, :] + block
                else:
                    col = (part * 2 + b) * BLK
                    acc[place, :] = start[:, col : col + BLK].astype(F32) + block

    for copy in loads[1:]:
        copy.wait()

    def own_step(q, carry):
        accumulate(q, at_own[...], own_v.at[q], res_v.at[q])
        return carry

    lax.fori_loop(0, quarters, own_step, 0)
    pass_word(2)
    for d in range(1, n_pair + 1):
        at_pair[d - 1, :, 0:tokens] = turned(lax.rem(z + n_z - d, n_z))
        at_pair[d - 1, :, tokens : 2 * tokens] = turned(lax.rem(z + d, n_z))
    at_far[...] = turned(lax.rem(z + n_z // 2, n_z))

    mask_loops = range(2, n_pair + 1) if n_pair > 1 else range(1, n_pair + 1)
    per_visit = -(-regions // (quarters * len(mask_loops)))
    row_of = lax.broadcasted_iota(jnp.int32, (rows, BLK), 0)
    col_of = lax.broadcasted_iota(jnp.int32, (BLK, BLK), 0)

    def mark(visit):
        total = hit[...]
        for i in range(per_visit):
            r = visit * per_visit + i
            in_row = jnp.where(row_of == rho[pl.ds(r, 1), :], 1.0, 0.0).astype(BF16)
            in_col = jnp.where(col_of == kappa[pl.ds(r, 1), :], 1.0, 0.0).astype(BF16)
            total = total + lax.dot_general(
                in_row, in_col, (((1,), (1,)), ((), ())), preferred_element_type=F32
            )
        hit[...] = total

    for d in range(1, n_pair + 1):

        def pair_step(q, carry, d=d):
            hop(0, d, q).wait_recv()
            hop(0, d + 1, q).start()
            hop(1, d, q).wait_recv()
            hop(1, d + 1, q).start()
            accumulate(q, at_pair[d - 1], pair.at[d - 1, q], None)
            if d in mask_loops:
                mark((d - mask_loops[0]) * quarters + q)
            return carry

        pass_word(d + 2)
        lax.fori_loop(0, quarters, pair_step, 0)

    def far_step(q, carry):
        hop(0, n_pair + 1, q).wait_recv()
        hop(1, n_pair + 1, q).wait_recv()
        accumulate(q, at_far[...], far.at[q], None)
        return carry

    for stage in range(n_pair + 3, len(stages) + 1):
        pass_word(stage)
    index_copy.wait()
    lax.fori_loop(0, quarters, far_step, 0)

    def far_first(k, n_rows, n_along):
        step = k // n_rows
        aside = (step + 1) // 2
        along = n_along // 2 + aside - 2 * aside * lax.rem(step, 2)
        return along + n_along * (n_rows - 1 - lax.rem(k, n_rows))

    half_rows = max(half // n_y, 1)

    def slot_of(k):
        return lax.rem(lane_row + far_first(k, half_rows, half // half_rows), half)

    def pick(base):
        got = []
        for i in range(own_tiles):
            begin = (base + i) * 8
            j = begin // regions
            for m in range(8):
                at = idx_s[j, begin - j * regions + m]
                at = jnp.minimum(jnp.maximum(at, 0), nowhere)
                got.append(acc[pl.ds(at, 1), :])
        for i in range(own_tiles):
            for m in range(8):
                contrib[base + i, m : m + 1, :] = got[8 * i + m]

    mine = core * half_tiles
    theirs = (1 - core) * half_tiles

    def to_partner(k):
        at = slot_of(k) * own_tiles
        return pltpu.make_async_remote_copy(
            src_ref=contrib.at[pl.ds(theirs + at, own_tiles)],
            dst_ref=partner_in.at[pl.ds(at, own_tiles)],
            send_sem=pair_send.at[k],
            recv_sem=pair_recv.at[k],
            device_id={"dp": partner, "tensor": z},
            device_id_type=MESH,
        )

    def scatter(k):
        slot = slot_of(k)
        return pltpu.make_async_remote_copy(
            src_ref=share.at[pl.ds(slot * own_tiles, own_tiles)],
            dst_ref=gathered.at[chip],
            send_sem=rs_send.at[k],
            recv_sem=rs_recv,
            device_id={"dp": 2 * (core * half + slot) + core, "tensor": z},
            device_id_type=MESH,
        )

    def partner_step(k, carry):
        pick(theirs + slot_of(k) * own_tiles)
        to_partner(k).start()
        return carry

    def share_piece(k):
        at = slot_of(k) * own_tiles
        pick(mine + at)
        to_partner(k).wait_recv()
        piece = pl.ds(at, own_tiles)
        share[piece] = contrib[pl.ds(mine + at, own_tiles)] + partner_in[piece]

    def scatter_step(k, carry):
        share_piece(k)
        scatter(k).start()
        return carry

    def both_step(k, carry):
        partner_step(k + ahead, carry)
        return scatter_step(k, carry)

    ahead = min(6, half)
    lax.fori_loop(0, ahead, partner_step, 0)
    lax.fori_loop(0, half - ahead, both_step, 0)
    lax.fori_loop(half - ahead, half - 1, scatter_step, 0)
    share_piece(half - 1)

    @pl.when(jnp.logical_not(owner))
    def _():
        scatter(half - 1).start()

    for c in range(n_cols):
        keep = hit[:, c : c + 1] < 0.5
        value = acc[c * rows : (c + 1) * rows, :]
        new_v[:, c * BLK : (c + 1) * BLK] = jnp.where(keep, value, 0.0).astype(BF16)

    def hand_out(k):
        return pltpu.make_async_remote_copy(
            src_ref=totals.at[pl.ds(chip * own_tiles, own_tiles)],
            dst_ref=totals.at[pl.ds(chip * own_tiles, own_tiles)],
            send_sem=ag_send,
            recv_sem=ag_recv,
            device_id={"dp": 2 * lax.rem(chip + far_first(k, n_x, n_y), chips) + core, "tensor": z},
            device_id_type=MESH,
        )

    def hand_step(k, carry):
        hand_out(k).start()
        return carry

    def wait_for(ref, count, sem):
        if count == 0:
            return
        part = ref.at[pl.ds(0, count)]
        pltpu.make_async_copy(part, part, sem).wait()

    @pl.when(owner)
    def _():
        gathered[chip] = share[pl.ds(lane_row * own_tiles, own_tiles)]
        wait_for(gathered, chips - 1, rs_recv)
        total = gathered[0]
        for k in range(1, chips):
            total = total + gathered[k]
        totals[pl.ds(chip * own_tiles, own_tiles)] = total
        lax.fori_loop(0, chips - 1, hand_step, 0)
        wait_for(totals, (half - 1) * own_tiles, ag_recv)

    @pl.when(jnp.logical_not(owner))
    def _():
        wait_for(totals, half_tiles, ag_recv)

    swap = pltpu.make_async_remote_copy(
        src_ref=totals.at[pl.ds(mine, half_tiles)],
        dst_ref=totals.at[pl.ds(mine, half_tiles)],
        send_sem=swap_send,
        recv_sem=swap_recv,
        device_id={"dp": partner, "tensor": z},
        device_id_type=MESH,
    )
    swap.start()

    for d in range(1, n_pair + 2):

        def sent_step(q, carry, d=d):
            hop(0, d, q).wait_send()
            hop(1, d, q).wait_send()
            return carry

        lax.fori_loop(0, quarters, sent_step, 0)

    def left_step(k, carry):
        to_partner(k).wait_send()
        return carry

    def scattered_step(k, carry):
        scatter(k).wait_send()
        return carry

    lax.fori_loop(0, half, left_step, 0)
    lax.fori_loop(0, half - 1, scattered_step, 0)

    @pl.when(jnp.logical_not(owner))
    def _():
        scatter(half - 1).wait_send()

    @pl.when(owner)
    def _():
        wait_for(totals, (chips - 1) * own_tiles, ag_send)

    swap.wait()
    kept_ref[...] = totals[...]


def finish(new_v, kept_v, new_out, kept_out, sems):
    copies = [
        pltpu.make_async_copy(kept_v, kept_out, sems.at[0]),
        pltpu.make_async_copy(new_v, new_out, sems.at[1]),
    ]
    for copy in copies:
        copy.start()
    for copy in copies:
        copy.wait()


def on_device(
    attn_out, cotangent, residual, local_offsets, local_counts, kept_offsets, kept_counts, bounds
):
    n_dp, n_z = lax.axis_size("dp"), lax.axis_size("tensor")
    chips = n_dp // 2
    n_y = GRID_Y if chips % GRID_Y == 0 else chips
    n_x = chips // n_y
    tokens, width = cotangent.shape
    rows = attn_out.shape[1]
    regions = local_offsets.shape[2]
    n_pair = n_z // 2 - 1
    quarters = width // CHUNK
    n_cols = width // BLK
    padded = -(-regions // 8) * 8 + 8 * quarters
    anywhere = pl.BlockSpec(memory_space=pl.ANY)
    vmem = pl.BlockSpec(memory_space=pltpu.VMEM)
    slots = local_offsets.shape[3]
    dma = pltpu.SemaphoreType.DMA
    tiles = regions * KEPT // 8
    new, kept = pl.pallas_call(
        functools.partial(kernel, {"chips": chips, "n_z": n_z, "n_x": n_x, "n_y": n_y}),
        out_shape=(
            pltpu.VMEM((rows, width), BF16),
            pltpu.VMEM((tiles, 8, BLK), F32),
        ),
        in_specs=[anywhere] * 8,
        out_specs=(vmem, vmem),
        scratch_shapes=[
            pltpu.VMEM((slots, regions), jnp.int32),
            pltpu.VMEM((1, regions), jnp.int32),
            pltpu.VMEM((KEPT, 1, regions), jnp.int32),
            pltpu.VMEM((1, regions), jnp.int32),
            pltpu.VMEM((1, regions + 1), jnp.int32),
            pltpu.VMEM(attn_out.shape, BF16),
            pltpu.VMEM((quarters, tokens, CHUNK), BF16),
            pltpu.VMEM((quarters, rows, CHUNK), BF16),
            pltpu.VMEM((rows, tokens), BF16),
            pltpu.VMEM((n_pair, rows, 2 * tokens), BF16),
            pltpu.VMEM((rows, tokens), BF16),
            pltpu.VMEM((n_pair, quarters, 2 * tokens, CHUNK), BF16),
            pltpu.VMEM((quarters, tokens, CHUNK), BF16),
            pltpu.VMEM((rows * n_cols + 8, BLK), F32),
            pltpu.VMEM((padded, BLK), jnp.int32),
            pltpu.VMEM((padded, BLK), jnp.int32),
            pltpu.VMEM((rows, BLK), F32),
            pltpu.VMEM((16, BLK), jnp.int32),
            pltpu.SMEM((16, BLK), jnp.int32),
            pltpu.VMEM((tiles, 8, BLK), F32),
            pltpu.VMEM((tiles // 2, 8, BLK), F32),
            pltpu.VMEM((tiles // 2, 8, BLK), F32),
            pltpu.VMEM((chips, tiles // chips, 8, BLK), F32),
            pltpu.VMEM((tiles, 8, BLK), F32),
            dma((5,)),
            dma((1 + 2 * quarters,)),
            dma,
            dma((2, n_pair + 1, quarters)),
            dma((2, n_pair + 1, quarters)),
            pltpu.SemaphoreType.REGULAR((n_x + n_y,)),
            dma((chips // 2,)),
            dma((chips // 2,)),
            dma((chips // 2,)),
            dma,
            dma,
            dma,
            dma,
            dma,
        ],
        compiler_params=pltpu.CompilerParams(collective_id=0, has_side_effects=True),
    )(
        attn_out,
        cotangent,
        residual[0],
        local_offsets[0, 0].T,
        local_counts[0],
        kept_offsets.transpose(2, 0, 1),
        kept_counts,
        bounds[None],
    )
    new = pltpu.with_memory_space_constraint(new, pltpu.VMEM)
    kept = pltpu.with_memory_space_constraint(kept, pltpu.VMEM)
    new, kept = pl.pallas_call(
        finish,
        out_shape=(
            jax.ShapeDtypeStruct(new.shape, BF16),
            jax.ShapeDtypeStruct(kept.shape, F32),
        ),
        in_specs=[vmem] * 2,
        out_specs=(anywhere, anywhere),
        scratch_shapes=[dma((2,))],
    )(new, kept)
    return new[None], kept.reshape(KEPT, regions, BLK).transpose(1, 0, 2)[None]


def solution(mesh):
    in_specs = (
        P("dp", "tensor"),
        P(("dp", "tensor"), None),
        P("dp", "tensor", None),
        P("dp", "tensor", None, None),
        P("dp", "tensor", None),
        P("tensor", None, None),
        P("tensor", None),
        P(),
    )
    out_specs = (P("dp", "tensor", None), P("tensor", None, None, None))
    return jax.shard_map(
        on_device, mesh=mesh, in_specs=in_specs, out_specs=out_specs, check_vma=False
    )
```
